512 devices in a mesh: learner: 16 (over y, x), rollout: 8 (over z_lo), dp: 4 (over z_hi, core).
Axes of the slice: x: 4, y: 4, z: 16 (z_hi: 2, z_lo: 8; z = z_hi * 8 + z_lo), core: 2. Of those that a mesh axis runs over, the one named last changes fastest.
Arguments:
- weight_delta: float32 [8192, 14336], P(('rollout', 'dp'), 'learner'), may hold values from -0.48 to 0.48
- sketch_seed: int32 [1], replicated, may hold values from 0 to 1048575
- up_weight: bfloat16 [8192, 14336], P('rollout', 'learner'), may hold values from -0.0625 to 0.0625
- down_weight: bfloat16 [14336, 8192], P('learner', 'rollout'), may hold values from -0.046875 to 0.046875
- norm_gain: bfloat16 [8192], P('rollout'), may hold values from 0.5 to 1.5
- state_pool: bfloat16 [128, 8192], P(None, 'rollout'), may hold values from -12 to 12
- token_rows: int32 [2, 4, 128], P(None, 'dp'), may hold values from 0 to 127
Outputs:
- decoded: bfloat16 [4, 128, 8192], P('dp', 'learner', 'rollout')
The draws below stay inside these ranges and needn't reach their ends.
All inputs are finite; a program needn't handle non-finite values.
Results may differ from the reference program's by a relative error of at most 0.017.
Values may be sent and summed in bfloat16 or wider, within the bound.
No kernel may reach another device: no remote copies, remote signals or barrier semaphores. Data moves between devices by JAX's collectives and lax.ppermute only.
A program may use at most 64 MiB of HBM per device.

```python
import jax
import jax.numpy as jnp
from jax import lax

D = 8192
FF = 14336
RANK = 128
ROWS = 128
POOL = 128
REPLICAS = 4


def draw_state_pool(key, part):
    first_key, second_key = jax.random.split(key, 2)
    col_scale = 3.0 ** (jnp.arange(D, dtype=jnp.float32) / D) * jax.random.uniform(second_key, (D,), jnp.float32, 0.6, 1.4)
    base = jax.random.normal(first_key, (POOL, D), jnp.float32)
    return jnp.clip(base * col_scale, -12.0, 12.0).astype(jnp.bfloat16)


def with_ends(result, stream_key, low, high):
    extent = result.shape
    place = [jax.random.randint(jax.random.fold_in(stream_key, axis), (), 0, extent[axis]) for axis in range(len(extent))]
    result = result.at[tuple(place)].set(low)
    longest = extent.index(max(extent))
    place[longest] = (place[longest] + 1) % extent[longest]
    return result.at[tuple(place)].set(high)


def level_of(key, extent, pieces, low, top_value):
    loudness, own = 1.0, jax.random.fold_in(key, 6)
    for position, parts in pieces:
        steps = jnp.exp(jax.random.uniform(jax.random.fold_in(own, position), (parts,), jnp.float32, low / len(pieces), top_value / len(pieces)))
        loudness = loudness * jnp.repeat(steps, extent[position] // parts).reshape([-1 if axis == position else 1 for axis in range(len(extent))])
    return loudness


def centred(rng, shape, spread, most, pieces=(), kind=jnp.bfloat16):
    loudness = level_of(rng, shape, pieces, -0.22, 0.18) if pieces else 1.0
    array = jax.random.normal(rng, shape, jnp.float32) * spread * loudness
    return jnp.minimum(jnp.maximum(array, -most), most).astype(kind)


def setup_inputs(seed: int = 0) -> dict:
    streams_of = jax.random.split(jax.random.key(seed), 8)
    return {
        "weight_delta": centred(streams_of[0], (D, FF), 0.06, 0.48, ((0, 32), (1, 16)), jnp.float32),
        "sketch_seed": jax.random.randint(streams_of[1], (1,), 0, 1048576).astype(jnp.int32),
        "up_weight": centred(streams_of[2], (D, FF), D ** -0.5, 0.0625, ((0, 8), (1, 16))),
        "down_weight": centred(streams_of[3], (FF, D), FF ** -0.5, 0.046875, ((0, 16), (1, 8))),
        "norm_gain": jnp.clip(1.0 + 0.1 * jax.random.normal(streams_of[4], (D,), jnp.float32), 0.5, 1.5).astype(jnp.bfloat16),
        "state_pool": draw_state_pool(jax.random.fold_in(streams_of[7], 71), 0),
        "token_rows": with_ends(jax.random.randint(streams_of[6], (2, REPLICAS, ROWS), 0, POOL), jax.random.fold_in(streams_of[6], 1), 0, POOL - 1).astype(jnp.int32),
    }


def sketch(sketch_seed, row_start, row_count, rank_count):
    row_index = row_start + lax.broadcasted_iota(jnp.int32, (row_count, rank_count), 0)
    col_index = lax.broadcasted_iota(jnp.int32, (row_count, rank_count), 1)
    hashed = row_index * rank_count + col_index + sketch_seed[0] * 7919
    hashed = hashed * 1103515245 + 12345
    hashed = hashed ^ lax.shift_right_logical(hashed, jnp.int32(16))
    hashed = hashed * 73244475
    hashed = hashed ^ lax.shift_right_logical(hashed, jnp.int32(15))
    parity = lax.shift_right_logical(hashed, jnp.int32(11)) & 1
    return (2 * parity - 1).astype(jnp.float32)

def apply_layer(inputs, weight_wide, down_wide, gain_values):
    values = inputs.astype(jnp.float32)
    mean_square = lax.optimization_barrier(jnp.mean(values * values, axis=-1, keepdims=True))
    normed = (values * lax.rsqrt(mean_square + 1e-05) * gain_values).astype(jnp.bfloat16)
    hidden = jax.nn.silu(jnp.dot(normed.astype(jnp.float32), weight_wide)).astype(jnp.bfloat16)
    return jnp.dot(hidden.astype(jnp.float32), down_wide)

def reference(weight_delta, sketch_seed, up_weight, down_weight, norm_gain, state_pool, token_rows):
    precise = lax.Precision.HIGHEST
    sketch_matrix = sketch(sketch_seed, 0, FF, RANK)
    range_basis = jnp.dot(weight_delta.astype(jnp.float32), sketch_matrix.astype(jnp.float32), precision=precise, preferred_element_type=jnp.float32)
    gram_matrix = jnp.dot(range_basis.T.astype(jnp.float32), range_basis.astype(jnp.float32), precision=precise, preferred_element_type=jnp.float32)
    lower_factor = jnp.linalg.cholesky(gram_matrix)
    ortho_basis = lax.linalg.triangular_solve(lower_factor, range_basis, left_side=False, lower=True, transpose_a=True)
    coefficients = jnp.dot(ortho_basis.T.astype(jnp.float32), weight_delta.astype(jnp.float32), precision=precise, preferred_element_type=jnp.float32)
    update = jnp.dot(ortho_basis.astype(jnp.float32), coefficients.astype(jnp.float32), precision=precise, preferred_element_type=jnp.float32)
    new_weight = (up_weight.astype(jnp.float32) + update).astype(jnp.bfloat16)
    weight_wide = new_weight.astype(jnp.float32)
    down_wide = down_weight.astype(jnp.float32)
    gain_values = norm_gain.astype(jnp.float32)
    pool_values = state_pool.astype(jnp.float32)

    def replica(picked):
        first_rows = state_pool[picked[0]]
        step_one = apply_layer(first_rows, weight_wide, down_wide, gain_values)
        carried = (first_rows.astype(jnp.float32) + step_one).astype(jnp.bfloat16)
        second_rows = (carried.astype(jnp.float32) + pool_values[picked[1]]).astype(jnp.bfloat16)
        step_two = apply_layer(second_rows, weight_wide, down_wide, gain_values)
        return (second_rows.astype(jnp.float32) + step_two).astype(jnp.bfloat16)
    return lax.map(replica, jnp.moveaxis(token_rows, 1, 0))
```

```python
import functools

import jax
import jax.numpy as jnp
from jax import lax
from jax.experimental import pallas as pl
from jax.experimental.pallas import tpu as pltpu
from jax.sharding import Mesh
from jax.sharding import PartitionSpec as P

D = 8192
RANK = 128
EPS = 1e-05
L = ("y", "x")
CL = ("c", "y", "x")
Z = ("zl", "zh")
BF = jnp.bfloat16
F32 = jnp.float32


def swap(x, axis):
    return lax.all_to_all(x, axis, split_axis=0, concat_axis=0, tiled=True)


def sent_to_all(x, axis):
    return swap(jnp.broadcast_to(x, (lax.axis_size(axis), *x.shape)), axis)


def summed(x, axis):
    count = lax.axis_size(axis)
    parts = swap(x.reshape(count, x.shape[0] // count, x.shape[1]), axis)
    return jnp.sum(parts.astype(F32), axis=0)


def dot(a, b):
    return jnp.dot(a, b, preferred_element_type=F32)


def dot_t(a, b):
    return lax.dot_general(a, b, (((0,), (0,)), ((), ())), preferred_element_type=F32)


def sketch(sketch_seed, row_start, row_count, rank_count):
    row_index = row_start + lax.broadcasted_iota(jnp.int32, (row_count, rank_count), 0)
    col_index = lax.broadcasted_iota(jnp.int32, (row_count, rank_count), 1)
    hashed = row_index * rank_count + col_index + sketch_seed[0] * 7919
    hashed = hashed * 1103515245 + 12345
    hashed = hashed ^ lax.shift_right_logical(hashed, jnp.int32(16))
    hashed = hashed * 73244475
    hashed = hashed ^ lax.shift_right_logical(hashed, jnp.int32(15))
    parity = lax.shift_right_logical(hashed, jnp.int32(11)) & 1
    return (2 * parity - 1).astype(F32)


def hi_lo(x):
    hi = lax.reduce_precision(x, 8, 7)
    return hi, x - hi


def diagonal_offset(rows, first):
    row = first + lax.broadcasted_iota(jnp.int32, (rows, RANK), 0)
    col = lax.broadcasted_iota(jnp.int32, (rows, RANK), 1)
    return (col - row) & (RANK - 1)


def precise(a, b):
    return jnp.dot(a, b, precision=lax.Precision.HIGHEST, preferred_element_type=F32)


def first_hidden_kernel(half, z_ref, hidden_ref, coef_ref, pre_ref):
    packed = z_ref[:, 2 * half : 2 * half + RANK].astype(F32)
    row = lax.broadcasted_iota(jnp.int32, (RANK, RANK), 0)
    col = lax.broadcasted_iota(jnp.int32, (RANK, RANK), 1)
    offset = (col - row) & (RANK - 1)
    squares = jnp.sum(jnp.where(offset >= RANK - 2, packed, 0.0), axis=1, keepdims=True)
    gram = jnp.where(offset <= RANK // 2, packed, packed.T)
    eye = jnp.where(row == col, 1.0, 0.0)
    on_diag = gram * eye
    scale_col = lax.rsqrt(jnp.sum(on_diag, axis=1, keepdims=True))
    scale_row = lax.rsqrt(jnp.sum(on_diag, axis=0, keepdims=True))
    unit = gram * scale_col * scale_row
    bound = jnp.max(jnp.sum(jnp.abs(unit), axis=1, keepdims=True), axis=0, keepdims=True)
    step = 2.0 / (1.0 + bound)
    start = step * (2.0 * eye - step * unit)

    def going(state):
        count, error, _ = state
        return jnp.logical_and(count < 40, error > 1e-5)

    def refine(state):
        count, _, inverse = state
        left = eye - precise(unit, inverse)
        return count + 1, jnp.sum(left * left), inverse + precise(inverse, left)

    _, _, inverse = lax.while_loop(going, refine, (0, jnp.float32(1.0), start))
    moved = z_ref[:, :half].astype(F32) * scale_col
    coef = (precise(inverse, moved) * scale_col).astype(BF)
    coef_ref[...] = coef
    total = z_ref[:, half : 2 * half].astype(F32) + jnp.dot(
        z_ref[:, 2 * half + RANK :], coef, preferred_element_type=F32
    )
    pre_ref[...] = total.astype(BF)
    pre = total * lax.rsqrt(squares / D + EPS)
    hidden_ref[...] = (pre / (1.0 + jnp.exp(-pre))).astype(BF)


def first_hidden(gathered, half):
    shape = jax.ShapeDtypeStruct((RANK, half), BF)
    return pl.pallas_call(
        functools.partial(first_hidden_kernel, half),
        out_shape=(shape, shape, shape),
        in_specs=[pl.BlockSpec(memory_space=pltpu.VMEM)],
        out_specs=(pl.BlockSpec(memory_space=pltpu.VMEM),) * 3,
    )(gathered)


def local(weight_delta, sketch_seed, up_weight, down_weight, norm_gain, state_pool, token_rows):
    core = lax.axis_index("c")
    z_half = lax.axis_index("zh")
    z_own = lax.axis_index(Z)
    learner = lax.axis_index(L)
    rows, cols = weight_delta.shape
    half = cols // 2
    width = 2 * rows
    pool_rows = state_pool.shape[0]

    def own_half(x):
        return jnp.where(core == 0, x[:, :half], x[:, half:])

    tokens = token_rows[:, 0, :].reshape(-1, 1)
    delta = weight_delta.astype(BF)
    kept = own_half(delta)
    other = jnp.where(core == 0, delta[:, half:], delta[:, :half])
    sent = jnp.concatenate([other, tokens.astype(BF)], axis=1)
    received = lax.ppermute(sent, "c", [(0, 1), (1, 0)])

    signs = sketch(sketch_seed, learner * cols, cols, RANK).astype(BF)
    range_share = summed(dot(delta, signs).astype(BF), L).astype(BF)
    basis = sent_to_all(range_share, CL).reshape(width, RANK)

    basis_own = lax.dynamic_slice_in_dim(basis, core * rows, rows, 0)
    basis_other = lax.dynamic_slice_in_dim(basis, (1 - core) * rows, rows, 0)
    other_tokens = received[:, half:].astype(jnp.int32)

    pool_half = lax.dynamic_slice_in_dim(state_pool, z_half * width, width, 1)
    gain_half = lax.dynamic_slice_in_dim(norm_gain, z_half * width, width, 0).astype(F32)
    up_half = lax.dynamic_slice_in_dim(up_weight, z_half * width, width, 0)
    down_half = lax.dynamic_slice_in_dim(down_weight, core * half, half, 0)

    pool_wide = pool_half.astype(F32)
    pool_gained = (pool_wide * gain_half).astype(BF)
    squares = jnp.sum(pool_wide * pool_wide, axis=1, keepdims=True)

    moved = dot_t(basis_own, kept) + dot_t(basis_other, received[:, :half])
    pool_up = own_half(dot(pool_gained, up_half))
    offset = diagonal_offset(RANK, 0)
    hi, lo = hi_lo(squares)

    def packed(gram, hi, lo, offset):
        rest = jnp.where(offset == RANK - 1, lo, jnp.where(offset == RANK - 2, hi, 0.0))
        return jnp.where(offset <= RANK // 2, gram, rest)

    gram = packed(dot_t(basis, basis), hi, lo, offset)
    pool_basis = dot(pool_gained, basis)
    stacked = jnp.concatenate([moved, pool_up, gram, pool_basis], axis=1).astype(BF)
    share = summed(stacked, Z)
    share_rows = share.shape[0]
    offset = diagonal_offset(share_rows, z_own * share_rows)
    gram = share[:, 2 * half : 2 * half + RANK]
    hi, lo = hi_lo(jnp.sum(jnp.where(offset >= RANK - 2, gram, 0.0), axis=1, keepdims=True))
    gram = packed(gram, hi, lo, offset)
    share = jnp.concatenate(
        [share[:, : 2 * half], gram, share[:, 2 * half + RANK :]], axis=1
    ).astype(BF)
    gathered = sent_to_all(share, Z).reshape(RANK, -1)

    hidden, coef, pool_pre = first_hidden(gathered, half)
    step_share = summed(dot(hidden, down_half).astype(BF), CL).astype(BF)
    step_one = sent_to_all(step_share, CL).reshape(pool_rows, -1)
    carried = (state_pool.astype(F32) + step_one.astype(F32)).astype(BF)
    carried_half = lax.dynamic_slice_in_dim(carried, z_half * width, width, 1)
    carried_gained = (carried_half.astype(F32) * gain_half).astype(BF)

    up_share = own_half(dot(carried_gained, up_half)) + dot(
        dot(carried_gained, basis).astype(BF), coef
    )

    first_core = jnp.where(core == 0, tokens, other_tokens)
    last_core = jnp.where(core == 0, other_tokens, tokens)
    count = pool_rows
    choice = lax.broadcasted_iota(jnp.int32, (2 * count, pool_rows), 1)

    def picks(step):
        span = slice(step * count, (step + 1) * count)
        both = jnp.concatenate([first_core[span], last_core[span]], axis=0)
        return (both == choice).astype(BF)

    pick_one, pick_two = picks(0), picks(1)
    second = (dot(pick_one, carried) + dot(pick_two, state_pool)).astype(BF).astype(F32)
    squares = jnp.sum(second * second, axis=1, keepdims=True)
    tail = jnp.concatenate([squares[:count], squares[count:]], axis=1)
    tail = jnp.concatenate(
        [jnp.where(z_half == 0, tail, 0.0), jnp.where(z_half == 1, tail, 0.0)], axis=1
    )
    blank = jnp.zeros((count, 4 * RANK - half - 8), F32)
    stacked = jnp.concatenate([up_share, *hi_lo(tail), blank], axis=1).astype(BF)
    share = summed(stacked, Z)
    tail = share[:, half : half + 4] + share[:, half + 4 : half + 8]
    share = jnp.concatenate([share[:, :half], *hi_lo(tail), share[:, half + 8 :]], axis=1)
    gathered = sent_to_all(share.astype(BF), Z).reshape(pool_rows, -1)
    tail = gathered[:, half : half + 8].astype(F32)
    tail = tail[:, :4] + tail[:, 4:]
    tail = jnp.where(z_half == 0, tail[:, :2], tail[:, 2:])
    squares = jnp.concatenate([tail[:, :1], tail[:, 1:]], axis=0)
    pre = dot(pick_one, gathered[:, :half]) + dot(pick_two, pool_pre)
    hidden = jax.nn.silu(pre * lax.rsqrt(squares / D + EPS)).astype(BF)
    last_share = summed(dot(hidden, down_half).astype(BF), CL)

    out_rows = last_share.shape[0]
    own = lax.dynamic_slice_in_dim(tokens, learner * out_rows, out_rows, 0)
    own_two = lax.dynamic_slice_in_dim(tokens, count + learner * out_rows, out_rows, 0)
    choice = lax.broadcasted_iota(jnp.int32, (out_rows, pool_rows), 1)
    own_second = (
        dot((own == choice).astype(BF), carried) + dot((own_two == choice).astype(BF), state_pool)
    ).astype(BF)
    return (own_second.astype(F32) + last_share).astype(BF)[None]


def solution(mesh):
    torus = Mesh(
        mesh.devices.reshape(4, 4, mesh.shape["rollout"], 2, 2), ("y", "x", "zl", "zh", "c")
    )
    return jax.shard_map(
        local,
        mesh=torus,
        in_specs=(
            P(("zl", "zh", "c"), L),
            P(),
            P("zl", L),
            P(L, "zl"),
            P("zl"),
            P(None, "zl"),
            P(None, ("zh", "c"), None),
        ),
        out_specs=P(("zh", "c"), L, "zl"),
        check_vma=False,
    )
```

```python
import functools

import jax
import jax.numpy as jnp
from jax import lax
from jax.experimental import pallas as pl
from jax.experimental.pallas import tpu as pltpu
from jax.sharding import Mesh
from jax.sharding import PartitionSpec as P

D = 8192
RANK = 128
EPS = 1e-05
L = ("y", "x")
CL = ("c", "y", "x")
Z = ("zl", "zh")
BF = jnp.bfloat16
F32 = jnp.float32


def swap(x, axis):
    return lax.all_to_all(x, axis, split_axis=0, concat_axis=0, tiled=True)


def sent_to_all(x, axis):
    return swap(jnp.broadcast_to(x, (lax.axis_size(axis), *x.shape)), axis)


def dot(a, b):
    return jnp.dot(a, b, preferred_element_type=F32)


def dot_t(a, b):
    return lax.dot_general(a, b, (((0,), (0,)), ((), ())), preferred_element_type=F32)


def hi_lo(x):
    hi = x.astype(BF).astype(F32)
    return hi, x - hi


def diagonal_offset(rows, first):
    row = first + lax.broadcasted_iota(jnp.int32, (rows, RANK), 0)
    col = lax.broadcasted_iota(jnp.int32, (rows, RANK), 1)
    return (col - row) & (RANK - 1)


def packed(gram, squares, offset):
    hi, lo = hi_lo(squares)
    rest = jnp.where(offset == RANK - 1, lo, jnp.where(offset == RANK - 2, hi, 0.0))
    return jnp.where(offset <= RANK // 2, gram, rest)


def unpacked_squares(gram, offset):
    return jnp.sum(jnp.where(offset >= RANK - 2, gram, 0.0), axis=1, keepdims=True)


def precise(a, b):
    return jnp.dot(a, b, precision=lax.Precision.HIGHEST, preferred_element_type=F32)


def silu(x):
    return x / (1.0 + jnp.exp(-x))


def total(ref):
    return jnp.sum(ref[...].astype(F32), axis=0)


def call(kernel, shapes, place, *arrays, limit=24):
    specs = [pl.BlockSpec(memory_space=pltpu.SMEM)]
    specs += [pl.BlockSpec(memory_space=pltpu.VMEM)] * len(arrays)
    return pl.pallas_call(
        kernel,
        out_shape=tuple(jax.ShapeDtypeStruct(shape, BF) for shape in shapes),
        in_specs=specs,
        out_specs=(pl.BlockSpec(memory_space=pltpu.VMEM),) * len(shapes),
        compiler_params=pltpu.CompilerParams(vmem_limit_bytes=limit * 1024 * 1024),
    )(place, *arrays)


def range_kernel(place, delta_ref, tokens_ref, part_ref, kept_ref, sent_ref):
    core = place[0]
    rows, cols = delta_ref.shape
    half = cols // 2
    row_index = place[3] + lax.broadcasted_iota(jnp.int32, (cols, RANK), 0)
    col_index = lax.broadcasted_iota(jnp.int32, (cols, RANK), 1)
    hashed = row_index * RANK + col_index + place[4]
    hashed = hashed * 1103515245 + 12345
    hashed = hashed ^ lax.shift_right_logical(hashed, jnp.int32(16))
    hashed = hashed * 73244475
    hashed = hashed ^ lax.shift_right_logical(hashed, jnp.int32(15))
    parity = lax.shift_right_logical(hashed, jnp.int32(11)) & 1
    signs = (2 * parity - 1).astype(F32).astype(BF)
    delta = delta_ref[...].astype(BF)
    part_ref[...] = dot(delta, signs).astype(BF).reshape(part_ref.shape)
    left, right = delta[:, :half], delta[:, half:]
    kept_ref[...] = jnp.where(core == 0, left, right)
    sent_ref[:, :half] = jnp.where(core == 0, right, left)
    spare = sent_ref.shape[1] - half
    sent_ref[:, half:] = jnp.broadcast_to(tokens_ref[...].astype(F32), (rows, spare)).astype(BF)


def moved_kernel(place, basis_ref, kept_ref, got_ref, pool_ref, up_ref, squares_ref, out_ref):
    core = place[0]
    rows, half = kept_ref.shape
    count = basis_ref.shape[0] // 2
    own = basis_ref[pl.ds(core * count, count)].reshape(rows, RANK)
    other = basis_ref[pl.ds((1 - core) * count, count)].reshape(rows, RANK)
    basis = basis_ref[...].reshape(2 * rows, RANK)

    def put(first, values):
        values = values.astype(BF)
        out_ref[:, :, first : first + values.shape[1]] = values.reshape(
            *out_ref.shape[:2], values.shape[1]
        )

    moved = dot_t(own, kept_ref[...]) + dot_t(other, got_ref[:, :half])
    both = jnp.concatenate([moved.astype(BF), up_ref[...]], axis=1)
    put(0, both)
    put(2 * half, packed(dot_t(basis, basis), squares_ref[...], diagonal_offset(RANK, 0)))
    put(2 * half + RANK, dot(pool_ref[...], basis))


def share_kernel(place, parts_ref, out_ref):
    share = total(parts_ref)
    rows, width = share.shape
    first = width - 2 * RANK
    offset = diagonal_offset(rows, place[2] * rows)
    gram = share[:, first : first + RANK]
    gram = packed(gram, unpacked_squares(gram, offset), offset)
    share = jnp.concatenate([share[:, :first], gram, share[:, first + RANK :]], axis=1)
    out_ref[...] = jnp.broadcast_to(share.astype(BF), out_ref.shape)


def first_kernel(place, z_ref, down_ref, step_ref, coef_ref, pre_ref):
    half = coef_ref.shape[1]
    gathered = z_ref[...].reshape(RANK, z_ref.shape[2])
    gram = gathered[:, 2 * half : 2 * half + RANK].astype(F32)
    row = lax.broadcasted_iota(jnp.int32, (RANK, RANK), 0)
    col = lax.broadcasted_iota(jnp.int32, (RANK, RANK), 1)
    offset = (col - row) & (RANK - 1)
    squares = unpacked_squares(gram, offset)
    gram = jnp.where(offset <= RANK // 2, gram, gram.T)
    eye = jnp.where(row == col, 1.0, 0.0)
    on_diag = gram * eye
    scale_col = lax.rsqrt(jnp.sum(on_diag, axis=1, keepdims=True))
    scale_row = lax.rsqrt(jnp.sum(on_diag, axis=0, keepdims=True))
    unit = gram * scale_col * scale_row
    bound = jnp.max(jnp.sum(jnp.abs(unit), axis=1, keepdims=True), axis=0, keepdims=True)
    step = 2.0 / (1.0 + bound)
    start = step * (2.0 * eye - step * unit)

    def going(state):
        count, error, _ = state
        return jnp.logical_and(count < 40, error > 2e-4)

    def refine(state):
        count, _, inverse = state
        left = eye - precise(unit, inverse)
        return count + 1, jnp.sum(left * left), inverse + precise(inverse, left)

    _, _, inverse = lax.while_loop(going, refine, (0, jnp.float32(1.0), start))
    moved = gathered[:, :half].astype(F32) * scale_col
    coef = (precise(inverse, moved) * scale_col).astype(BF)
    coef_ref[...] = coef
    pre = gathered[:, half : 2 * half].astype(F32) + dot(gathered[:, 2 * half + RANK :], coef)
    pre_ref[...] = pre.astype(BF)
    hidden = silu(pre * lax.rsqrt(squares / D + EPS)).astype(BF)
    result = dot(hidden, down_ref[...]).astype(BF)
    count, rows, width = step_ref.shape
    step_ref[: count // 2] = result[:, :width].reshape(count // 2, rows, width)
    step_ref[count // 2 :] = result[:, width:].reshape(count // 2, rows, width)


def second_kernel(
    place, step_ref, pool_ref, gain_ref, up_ref, basis_ref, coef_ref, pick_ref, own_ref, out_ref, rows_ref
):
    z_half = place[1]
    count, rows, width = step_ref.shape
    pool_rows = pool_ref.shape[0]
    half = coef_ref.shape[1]
    basis = basis_ref[...].reshape(width, RANK)
    step = step_ref[...].astype(F32).reshape(2, pool_rows, width)
    pool = pool_ref[...]
    left = (pool[:, :width].astype(F32) + step[0]).astype(BF)
    right = (pool[:, width:].astype(F32) + step[1]).astype(BF)
    carried = jnp.concatenate([left, right], axis=1)
    gained = jnp.where(z_half == 0, left, right).astype(F32) * gain_ref[...]
    gained = gained.astype(BF)
    up = dot(gained, up_ref[...]) + dot(dot(gained, basis).astype(BF), coef_ref[...])

    def second(pick):
        return (dot(pick[0], carried) + dot(pick[1], pool)).astype(BF)

    wide = second(pick_ref).astype(F32)
    squares = jnp.sum(wide * wide, axis=1, keepdims=True)
    lane = lax.broadcasted_iota(jnp.int32, (pool_rows, out_ref.shape[2] - half), 1)
    first = 4 * z_half
    tail = jnp.zeros(lane.shape, F32)
    for place_in, value in enumerate((*hi_lo(squares[:pool_rows]), *hi_lo(squares[pool_rows:]))):
        tail = jnp.where(lane == first + place_in, value, tail)
    both = jnp.concatenate([up.astype(BF), tail.astype(BF)], axis=1)
    out_ref[...] = both.reshape(out_ref.shape)
    rows_ref[...] = second(own_ref)


def second_share_kernel(half, place, parts_ref, out_ref):
    share = total(parts_ref)
    lane = lax.broadcasted_iota(jnp.int32, share.shape, 1)
    out = share
    for first in range(half, half + 8, 2):
        whole = jnp.where(jnp.logical_or(lane == first, lane == first + 1), share, 0.0)
        hi, lo = hi_lo(jnp.sum(whole, axis=1, keepdims=True))
        out = jnp.where(lane == first, hi, jnp.where(lane == first + 1, lo, out))
    out_ref[...] = jnp.broadcast_to(out.astype(BF), out_ref.shape)


def last_kernel(place, z_ref, pre_ref, pick_ref, down_ref, out_ref):
    z_half = place[1]
    half = pre_ref.shape[1]
    pool_rows = pre_ref.shape[0]
    gathered = z_ref[...].reshape(pool_rows, z_ref.shape[2])
    lane = lax.broadcasted_iota(jnp.int32, gathered.shape, 1)

    def squares(first):
        first = half + 4 * z_half + first
        chosen = jnp.logical_or(lane == first, lane == first + 1)
        return jnp.sum(jnp.where(chosen, gathered.astype(F32), 0.0), axis=1, keepdims=True)

    scale = lax.rsqrt(jnp.concatenate([squares(0), squares(2)], axis=0) / D + EPS)
    pre = dot(pick_ref[0], gathered[:, :half]) + dot(pick_ref[1], pre_ref[...])
    hidden = silu(pre * scale).astype(BF)
    out_ref[...] = dot(hidden, down_ref[...]).astype(BF).reshape(out_ref.shape)


def local(weight_delta, sketch_seed, up_weight, down_weight, norm_gain, state_pool, token_rows):
    core = lax.axis_index("c")
    z_half = lax.axis_index("zh")
    learner = lax.axis_index(L)
    rows, cols = weight_delta.shape
    half = cols // 2
    width = 2 * rows
    count = state_pool.shape[0]
    out_rows = count // 16
    place = jnp.stack(
        [core, z_half, lax.axis_index(Z), learner * cols, sketch_seed[0] * 7919]
    ).astype(jnp.int32)

    tokens = token_rows[:, 0, :]
    part, kept, sent = call(
        range_kernel,
        ((16, rows // 16, RANK), (rows, half), (rows, half + 64)),
        place,
        weight_delta,
        tokens.reshape(-1, 1),
    )
    received = lax.ppermute(sent, "c", [(0, 1), (1, 0)])
    parts = swap(part, L)

    def own_half(x):
        return jnp.where(core == 0, x[:, :half], x[:, half:])

    pool_half = lax.dynamic_slice_in_dim(state_pool, z_half * width, width, 1).astype(F32)
    gain_half = lax.dynamic_slice_in_dim(norm_gain, z_half * width, width, 0).astype(F32)[None]
    up_own = own_half(lax.dynamic_slice_in_dim(up_weight, z_half * width, width, 0))
    down_own = lax.dynamic_slice_in_dim(down_weight, core * half, half, 0)
    pool_gained = (pool_half * gain_half).astype(BF)
    pool_up = dot(pool_gained, up_own).astype(BF)
    squares = jnp.sum(pool_half * pool_half, axis=1, keepdims=True)
    mine = tokens[:, :, None]
    theirs = received[:, half : half + 1].astype(jnp.int32).reshape(2, count, 1)
    both = jnp.where(
        core == 0, jnp.concatenate([mine, theirs], 1), jnp.concatenate([theirs, mine], 1)
    )
    picks = (both == lax.broadcasted_iota(jnp.int32, (2, 2 * count, count), 2)).astype(BF)
    own = lax.dynamic_slice_in_dim(mine, learner * out_rows, out_rows, 1)
    own_picks = (own == lax.broadcasted_iota(jnp.int32, (2, out_rows, count), 2)).astype(BF)

    range_share = jnp.sum(parts.astype(F32), axis=0).astype(BF)
    side = (kept, received, pool_gained, pool_up, squares, gain_half, up_own, down_own, picks, own_picks, place, state_pool)
    range_share, side = lax.optimization_barrier((range_share, side))
    kept, received, pool_gained, pool_up, squares, gain_half, up_own, down_own, picks, own_picks, place, pool = side

    basis = sent_to_all(range_share, CL)
    (stacked,) = call(
        moved_kernel,
        ((16, count // 16, 2 * half + 2 * RANK),),
        place, basis, kept, received, pool_gained, pool_up, squares,
    )
    (share,) = call(share_kernel, (stacked.shape,), place, swap(stacked, Z))
    step_part, coef, pool_pre = call(
        first_kernel,
        ((32, count // 16, width), (RANK, half), (count, half)),
        place, swap(share, Z), down_own,
    )
    step_share = jnp.sum(swap(step_part, CL).astype(F32), axis=0).astype(BF)
    step = sent_to_all(step_share, CL)
    stacked, own_second = call(
        second_kernel,
        ((16, count // 16, half + 64), (out_rows, 2 * width)),
        place, step, pool, gain_half, up_own, basis, coef, picks, own_picks,
    )
    (share,) = call(
        functools.partial(second_share_kernel, half), (stacked.shape,), place, swap(stacked, Z)
    )
    (last,) = call(
        last_kernel,
        ((32, out_rows, 2 * width),),
        place, swap(share, Z), pool_pre, picks, down_own,
    )
    last_share = jnp.sum(swap(last, CL).astype(F32), axis=0)
    return (own_second.astype(F32) + last_share).astype(BF)[None]


def solution(mesh):
    torus = Mesh(
        mesh.devices.reshape(4, 4, mesh.shape["rollout"], 2, 2), ("y", "x", "zl", "zh", "c")
    )
    return jax.shard_map(
        local,
        mesh=torus,
        in_specs=(
            P(("zl", "zh", "c"), L),
            P(),
            P("zl", L),
            P(L, "zl"),
            P("zl"),
            P(None, "zl"),
            P(None, ("zh", "c"), None),
        ),
        out_specs=P(("zh", "c"), L, "zl"),
        check_vma=False,
    )
```

```python
import functools

import jax
import jax.numpy as jnp
from jax import lax
from jax.experimental import pallas as pl
from jax.experimental.pallas import tpu as pltpu
from jax.sharding import Mesh
from jax.sharding import PartitionSpec as P

D = 8192
RANK = 128
EPS = 1e-05
L = ("y", "x")
CL = ("c", "y", "x")
Z = ("zl", "zh")
BF = jnp.bfloat16
F32 = jnp.float32


def swap(x, axis):
    return lax.all_to_all(x, axis, split_axis=0, concat_axis=0, tiled=True)


def sent_to_all(x, axis):
    return swap(jnp.broadcast_to(x, (lax.axis_size(axis), *x.shape)), axis)


def dot(a, b):
    return jnp.dot(a, b, preferred_element_type=F32)


def dot_t(a, b):
    return lax.dot_general(a, b, (((0,), (0,)), ((), ())), preferred_element_type=F32)


def hi_lo(x):
    hi = x.astype(BF).astype(F32)
    return hi, x - hi


def diagonal_offset(rows, first):
    row = first + lax.broadcasted_iota(jnp.int32, (rows, RANK), 0)
    col = lax.broadcasted_iota(jnp.int32, (rows, RANK), 1)
    return (col - row) & (RANK - 1)


def packed(gram, squares, offset):
    hi, lo = hi_lo(squares)
    rest = jnp.where(offset == RANK - 1, lo, jnp.where(offset == RANK - 2, hi, 0.0))
    return jnp.where(offset <= RANK // 2, gram, rest)


def unpacked_squares(gram, offset):
    return jnp.sum(jnp.where(offset >= RANK - 2, gram, 0.0), axis=1, keepdims=True)


def precise(a, b):
    return jnp.dot(a, b, precision=lax.Precision.HIGHEST, preferred_element_type=F32)


def silu(x):
    return x / (1.0 + jnp.exp(-x))


def total(ref):
    return jnp.sum(ref[...].astype(F32), axis=0)


HBM = pl.BlockSpec(memory_space=pltpu.HBM)
VMEM = pl.BlockSpec(memory_space=pltpu.VMEM)


def call(kernel, shapes, place, *arrays, hbm=None, scratch=()):
    specs = [pl.BlockSpec(memory_space=pltpu.SMEM)]
    if hbm is not None:
        arrays = (hbm, *arrays)
        specs += [HBM]
        scratch = (*scratch, pltpu.SemaphoreType.DMA((2,)))
    specs += [VMEM] * (len(arrays) - (hbm is not None))
    return pl.pallas_call(
        kernel,
        out_shape=tuple(jax.ShapeDtypeStruct(shape, BF) for shape in shapes),
        in_specs=specs,
        out_specs=(VMEM,) * len(shapes),
        scratch_shapes=scratch,
        compiler_params=pltpu.CompilerParams(vmem_limit_bytes=16 * 1024 * 1024),
    )(place, *arrays)


def column(row):
    return jnp.broadcast_to(row, (RANK, RANK)).T


def chosen(tokens, step):
    count = tokens.shape[0] // 2
    rows = tokens[step * count : (step + 1) * count].astype(F32)
    lane = lax.broadcasted_iota(jnp.int32, (count, RANK), 1).astype(F32)
    return jnp.where(rows == lane, 1.0, 0.0).astype(BF)


def picks(place, kept_ref, got_ref, step):
    half = kept_ref.shape[1] - RANK // 2
    mine = chosen(kept_ref[:, half : half + 1], step)
    theirs = chosen(got_ref[:, half : half + 1], step)
    first = place[0] == 0
    return jnp.concatenate(
        [jnp.where(first, mine, theirs), jnp.where(first, theirs, mine)], axis=0
    )


def own_half(place, x):
    half = x.shape[1] // 2
    return jnp.where(place[0] == 0, x[:, :half], x[:, half:])


def range_kernel(place, delta_hbm, tokens_ref, part_ref, kept_ref, sent_ref, delta_ref, sem):
    core = place[0]
    rows, cols = delta_ref.shape
    half = cols // 2
    split = rows // 2
    copies = [
        pltpu.make_async_copy(
            delta_hbm.at[pl.ds(i * split, split)], delta_ref.at[pl.ds(i * split, split)], sem.at[i]
        )
        for i in range(2)
    ]
    for copy in copies:
        copy.start()
    row_index = place[3] + lax.broadcasted_iota(jnp.int32, (cols, RANK), 0)
    col_index = lax.broadcasted_iota(jnp.int32, (cols, RANK), 1)
    hashed = row_index * RANK + col_index + place[4]
    hashed = hashed * 1103515245 + 12345
    hashed = hashed ^ lax.shift_right_logical(hashed, jnp.int32(16))
    hashed = hashed * 73244475
    hashed = hashed ^ lax.shift_right_logical(hashed, jnp.int32(15))
    parity = lax.shift_right_logical(hashed, jnp.int32(11)) & 1
    signs = (2 * parity - 1).astype(F32).astype(BF)
    for i, copy in enumerate(copies):
        copy.wait()
        span = slice(i * split, (i + 1) * split)
        delta = delta_ref[span].astype(BF)
        parts = part_ref.shape[0] // 2
        part_ref[i * parts : (i + 1) * parts] = (
            dot(delta, signs).astype(BF).reshape(parts, *part_ref.shape[1:])
        )
        left, right = delta[:, :half], delta[:, half:]
        tokens = column(tokens_ref[i : i + 1].astype(F32))[:, : RANK // 2].astype(BF)
        kept_ref[span] = jnp.concatenate([jnp.where(core == 0, left, right), tokens], axis=1)
        sent_ref[span] = jnp.concatenate([jnp.where(core == 0, right, left), tokens], axis=1)


def pool_kernel(place, up_hbm, pool_ref, gain_ref, gained_ref, up_out_ref, squares_ref, up_ref, sem):
    z_half = place[1]
    width = up_ref.shape[0]
    first = pl.multiple_of(z_half * width, width)
    copy = pltpu.make_async_copy(up_hbm.at[pl.ds(first, width)], up_ref, sem.at[0])
    copy.start()
    pool = jnp.where(z_half == 0, pool_ref[:, :width], pool_ref[:, width:]).astype(F32)
    gain = jnp.where(z_half == 0, gain_ref[:, :width], gain_ref[:, width:])
    gained = (pool * gain).astype(BF)
    gained_ref[...] = gained
    squares = jnp.broadcast_to(jnp.sum(pool * pool, axis=1, keepdims=True), (pool.shape[0], RANK))
    hi, lo = hi_lo(squares)
    squares_ref[0] = hi.astype(BF)
    squares_ref[1] = lo.astype(BF)
    copy.wait()
    up_out_ref[...] = own_half(place, dot(gained, up_ref[...])).astype(BF)


def spread_kernel(place, parts_ref, out_ref):
    out_ref[...] = jnp.broadcast_to(total(parts_ref).astype(BF), out_ref.shape)


def moved_kernel(place, basis_ref, kept_ref, got_ref, pool_ref, up_ref, squares_ref, out_ref):
    core = place[0]
    rows, wide = kept_ref.shape
    half = wide - RANK // 2
    count = basis_ref.shape[0] // 2
    own = basis_ref[pl.ds(core * count, count)].reshape(rows, RANK)
    other = basis_ref[pl.ds((1 - core) * count, count)].reshape(rows, RANK)
    basis = basis_ref[...].reshape(2 * rows, RANK)

    def put(first, values):
        values = values.astype(BF)
        out_ref[:, :, first : first + values.shape[1]] = values.reshape(
            *out_ref.shape[:2], values.shape[1]
        )

    moved = dot_t(own, kept_ref[...]) + dot_t(other, got_ref[...])
    put(0, jnp.concatenate([moved[:, :half].astype(BF), up_ref[...]], axis=1))
    squares = squares_ref[0].astype(F32) + squares_ref[1].astype(F32)
    put(2 * half, packed(dot_t(basis, basis), squares, diagonal_offset(RANK, 0)))
    put(2 * half + RANK, dot(pool_ref[...], basis))


def share_kernel(place, parts_ref, out_ref):
    share = total(parts_ref)
    rows, width = share.shape
    first = width - 2 * RANK
    offset = diagonal_offset(rows, place[2] * rows)
    gram = share[:, first : first + RANK]
    gram = packed(gram, unpacked_squares(gram, offset), offset)
    share = jnp.concatenate([share[:, :first], gram, share[:, first + RANK :]], axis=1)
    out_ref[...] = jnp.broadcast_to(share.astype(BF), out_ref.shape)


def down_copy(place, down_hbm, down_ref, sem):
    half = down_ref.shape[0]
    first = pl.multiple_of(place[0] * half, RANK // 2)
    return pltpu.make_async_copy(down_hbm.at[pl.ds(first, half)], down_ref, sem.at[0])


def first_kernel(place, down_hbm, z_ref, step_ref, coef_ref, pre_ref, down_ref, sem):
    copy = down_copy(place, down_hbm, down_ref, sem)
    copy.start()
    half = coef_ref.shape[1]
    gathered = z_ref[...].reshape(RANK, z_ref.shape[2])
    gram = gathered[:, 2 * half : 2 * half + RANK].astype(F32)
    row = lax.broadcasted_iota(jnp.int32, (RANK, RANK), 0)
    col = lax.broadcasted_iota(jnp.int32, (RANK, RANK), 1)
    offset = (col - row) & (RANK - 1)
    squares = unpacked_squares(gram, offset)
    gram = jnp.where(offset <= RANK // 2, gram, gram.T)
    eye = jnp.where(row == col, 1.0, 0.0)
    on_diag = gram * eye
    scale_col = lax.rsqrt(jnp.sum(on_diag, axis=1, keepdims=True))
    scale_row = lax.rsqrt(jnp.sum(on_diag, axis=0, keepdims=True))
    unit = gram * scale_col * scale_row
    bound = jnp.max(jnp.sum(jnp.abs(unit), axis=1, keepdims=True), axis=0, keepdims=True)
    step = 2.0 / (1.0 + bound)
    start = step * (2.0 * eye - step * unit)

    def going(state):
        count, error, _ = state
        return jnp.logical_and(count < 40, error > 2e-4)

    def refine(state):
        count, _, inverse = state
        left = eye - precise(unit, inverse)
        return count + 1, jnp.sum(left * left), inverse + precise(inverse, left)

    _, _, inverse = lax.while_loop(going, refine, (0, jnp.float32(1.0), start))
    moved = gathered[:, :half].astype(F32) * scale_col
    coef = (precise(inverse, moved) * scale_col).astype(BF)
    coef_ref[...] = coef
    pre = gathered[:, half : 2 * half].astype(F32) + dot(gathered[:, 2 * half + RANK :], coef)
    pre_ref[...] = pre.astype(BF)
    hidden = silu(pre * lax.rsqrt(squares / D + EPS)).astype(BF)
    copy.wait()
    result = dot(hidden, down_ref[...]).astype(BF)
    count, rows, width = step_ref.shape
    step_ref[: count // 2] = result[:, :width].reshape(count // 2, rows, width)
    step_ref[count // 2 :] = result[:, width:].reshape(count // 2, rows, width)


def second_kernel(
    place, up_hbm, step_ref, pool_ref, gain_ref, basis_ref, coef_ref, kept_ref, got_ref, out_ref, rows_ref, up_ref, sem
):
    z_half = place[1]
    count, rows, width = step_ref.shape
    pool_rows = pool_ref.shape[0]
    start = pl.multiple_of(z_half * width, width)
    copy = pltpu.make_async_copy(up_hbm.at[pl.ds(start, width)], up_ref, sem.at[0])
    copy.start()
    half = coef_ref.shape[1]
    basis = basis_ref[...].reshape(width, RANK)
    step = step_ref[...].astype(F32).reshape(2, pool_rows, width)
    pool = pool_ref[...]
    left = (pool[:, :width].astype(F32) + step[0]).astype(BF)
    right = (pool[:, width:].astype(F32) + step[1]).astype(BF)
    carried = jnp.concatenate([left, right], axis=1)
    gain = jnp.where(z_half == 0, gain_ref[:, :width], gain_ref[:, width:])
    gained = (jnp.where(z_half == 0, left, right).astype(F32) * gain).astype(BF)

    def second(one, two):
        return (dot(one, carried) + dot(two, pool)).astype(BF)

    wide = second(
        picks(place, kept_ref, got_ref, 0), picks(place, kept_ref, got_ref, 1)
    ).astype(F32)
    squares = jnp.sum(wide * wide, axis=1, keepdims=True)
    row = lax.broadcasted_iota(jnp.int32, (rows_ref.shape[0], pool_rows), 0)
    lane = lax.broadcasted_iota(jnp.int32, (rows_ref.shape[0], pool_rows), 1)
    here = jnp.where(lane == row + place[5], 1.0, 0.0).astype(BF)
    tokens = kept_ref[:, half : half + 1]
    rows_ref[...] = second(
        dot(here, chosen(tokens, 0)).astype(BF), dot(here, chosen(tokens, 1)).astype(BF)
    )
    lane = lax.broadcasted_iota(jnp.int32, (pool_rows, out_ref.shape[2] - half), 1)
    first = 4 * z_half
    tail = jnp.zeros(lane.shape, F32)
    for place_in, value in enumerate((*hi_lo(squares[:pool_rows]), *hi_lo(squares[pool_rows:]))):
        tail = jnp.where(lane == first + place_in, value, tail)
    low = dot(dot(gained, basis).astype(BF), coef_ref[...])
    copy.wait()
    up = own_half(place, dot(gained, up_ref[...])) + low
    both = jnp.concatenate([up.astype(BF), tail.astype(BF)], axis=1)
    out_ref[...] = both.reshape(out_ref.shape)


def second_share_kernel(half, place, parts_ref, out_ref):
    share = total(parts_ref)
    lane = lax.broadcasted_iota(jnp.int32, share.shape, 1)
    out = share
    for first in range(half, half + 8, 2):
        whole = jnp.where(jnp.logical_or(lane == first, lane == first + 1), share, 0.0)
        hi, lo = hi_lo(jnp.sum(whole, axis=1, keepdims=True))
        out = jnp.where(lane == first, hi, jnp.where(lane == first + 1, lo, out))
    out_ref[...] = jnp.broadcast_to(out.astype(BF), out_ref.shape)


def last_kernel(place, down_hbm, z_ref, pre_ref, kept_ref, got_ref, out_ref, down_ref, sem):
    copy = down_copy(place, down_hbm, down_ref, sem)
    copy.start()
    z_half = place[1]
    half = pre_ref.shape[1]
    pool_rows = pre_ref.shape[0]
    gathered = z_ref[...].reshape(pool_rows, z_ref.shape[2])
    lane = lax.broadcasted_iota(jnp.int32, gathered.shape, 1)

    def squares(first):
        first = half + 4 * z_half + first
        chosen = jnp.logical_or(lane == first, lane == first + 1)
        return jnp.sum(jnp.where(chosen, gathered.astype(F32), 0.0), axis=1, keepdims=True)

    scale = lax.rsqrt(jnp.concatenate([squares(0), squares(2)], axis=0) / D + EPS)
    one, two = picks(place, kept_ref, got_ref, 0), picks(place, kept_ref, got_ref, 1)
    pre = dot(one, gathered[:, :half]) + dot(two, pre_ref[...])
    hidden = silu(pre * scale).astype(BF)
    copy.wait()
    out_ref[...] = dot(hidden, down_ref[...]).astype(BF).reshape(out_ref.shape)


def local(weight_delta, sketch_seed, up_weight, down_weight, norm_gain, state_pool, token_rows):
    learner = lax.axis_index(L)
    rows, cols = weight_delta.shape
    half = cols // 2
    width = 2 * rows
    count = state_pool.shape[0]
    out_rows = count // 16
    place = jnp.stack(
        [
            lax.axis_index("c"),
            lax.axis_index("zh"),
            lax.axis_index(Z),
            learner * cols,
            sketch_seed[0] * 7919,
            learner * out_rows,
        ]
    ).astype(jnp.int32)
    padded = half + RANK // 2
    part, kept, sent = call(
        range_kernel,
        ((16, rows // 16, RANK), (rows, padded), (rows, padded)),
        place,
        token_rows[:, 0, :],
        hbm=weight_delta,
        scratch=(pltpu.VMEM((rows, cols), F32),),
    )
    received = lax.ppermute(sent, "c", [(0, 1), (1, 0)])
    parts = swap(part, L)
    gain = norm_gain.astype(F32)[None]
    up_scratch = (pltpu.VMEM((width, cols), BF),)
    down_scratch = (pltpu.VMEM((half, 2 * width), BF),)
    gained, pool_up, squares = call(
        pool_kernel,
        ((count, width), (count, half), (2, count, RANK)),
        place, state_pool, gain,
        hbm=up_weight, scratch=up_scratch,
    )
    parts, received, gained, pool_up, squares, kept, place, gain, pool = lax.optimization_barrier(
        (parts, received, gained, pool_up, squares, kept, place, gain, state_pool)
    )
    (spread,) = call(spread_kernel, ((32, rows // 16, RANK),), place, parts)
    basis = swap(spread, CL)
    (stacked,) = call(
        moved_kernel,
        ((16, count // 16, 2 * half + 2 * RANK),),
        place, basis, kept, received, gained, pool_up, squares,
    )
    (share,) = call(share_kernel, (stacked.shape,), place, swap(stacked, Z))
    step_part, coef, pool_pre = call(
        first_kernel,
        ((32, count // 16, width), (RANK, half), (count, half)),
        place, swap(share, Z),
        hbm=down_weight, scratch=down_scratch,
    )
    (spread,) = call(spread_kernel, (step_part.shape,), place, swap(step_part, CL))
    step = swap(spread, CL)
    stacked, own_second = call(
        second_kernel,
        ((16, count // 16, padded), (out_rows, 2 * width)),
        place, step, pool, gain, basis, coef, kept, received,
        hbm=up_weight, scratch=up_scratch,
    )
    (share,) = call(
        functools.partial(second_share_kernel, half), (stacked.shape,), place, swap(stacked, Z)
    )
    (last,) = call(
        last_kernel,
        ((32, out_rows, 2 * width),),
        place, swap(share, Z), pool_pre, kept, received,
        hbm=down_weight, scratch=down_scratch,
    )
    last_share = jnp.sum(swap(last, CL).astype(F32), axis=0)
    return (own_second.astype(F32) + last_share).astype(BF)[None]


def solution(mesh):
    torus = Mesh(
        mesh.devices.reshape(4, 4, mesh.shape["rollout"], 2, 2), ("y", "x", "zl", "zh", "c")
    )
    return jax.shard_map(
        local,
        mesh=torus,
        in_specs=(
            P(("zl", "zh", "c"), L),
            P(),
            P("zl", L),
            P(L, "zl"),
            P("zl"),
            P(None, "zl"),
            P(None, ("zh", "c"), None),
        ),
        out_specs=P(("zh", "c"), L, "zl"),
        check_vma=False,
    )
```

```python
import functools

import jax
import jax.numpy as jnp
from jax import lax
from jax.experimental import pallas as pl
from jax.experimental.pallas import tpu as pltpu
from jax.sharding import Mesh
from jax.sharding import PartitionSpec as P


D = 8192
RANK = 128
EPS = 1e-05
L = ("y", "x")
CL = ("c", "y", "x")
Z = ("zl", "zh")
BF = jnp.bfloat16
F32 = jnp.float32


def swap(x, axis):
    return lax.all_to_all(x, axis, split_axis=0, concat_axis=0, tiled=True)


def dot(a, b):
    return jnp.dot(a, b, preferred_element_type=F32)


def dot_t(a, b):
    return lax.dot_general(a, b, (((0,), (0,)), ((), ())), preferred_element_type=F32)


def hi_lo(x):
    hi = x.astype(BF).astype(F32)
    return hi, x - hi


def diagonal_offset(rows, first):
    row = first + lax.broadcasted_iota(jnp.int32, (rows, RANK), 0)
    col = lax.broadcasted_iota(jnp.int32, (rows, RANK), 1)
    return (col - row) & (RANK - 1)


def packed(gram, squares, offset):
    hi, lo = hi_lo(squares)
    rest = jnp.where(offset == RANK - 1, lo, jnp.where(offset == RANK - 2, hi, 0.0))
    return jnp.where(offset <= RANK // 2, gram, rest)


def unpacked_squares(gram, offset):
    return jnp.sum(jnp.where(offset >= RANK - 2, gram, 0.0), axis=1, keepdims=True)


def precise(a, b):
    return jnp.dot(a, b, precision=lax.Precision.HIGHEST, preferred_element_type=F32)


def silu(x):
    return x / (1.0 + jnp.exp(-x))


def total(ref):
    return jnp.sum(ref[...].astype(F32), axis=0)


HBM = pl.BlockSpec(memory_space=pltpu.HBM)
VMEM = pl.BlockSpec(memory_space=pltpu.VMEM)


def call(kernel, shapes, place, *arrays, hbm=None, scratch=(), limit=16):
    specs = [pl.BlockSpec(memory_space=pltpu.SMEM)]
    if hbm is not None:
        arrays = (hbm, *arrays)
        specs += [HBM]
        scratch = (*scratch, pltpu.SemaphoreType.DMA((2,)))
    specs += [VMEM] * (len(arrays) - (hbm is not None))
    return pl.pallas_call(
        kernel,
        out_shape=tuple(jax.ShapeDtypeStruct(shape, BF) for shape in shapes),
        in_specs=specs,
        out_specs=(VMEM,) * len(shapes),
        scratch_shapes=scratch,
        compiler_params=pltpu.CompilerParams(vmem_limit_bytes=int(limit * 1024 * 1024)),
    )(place, *arrays)


def column(row):
    return jnp.broadcast_to(row, (RANK, RANK)).T


def chosen(tokens, step):
    count = tokens.shape[0] // 2
    rows = tokens[step * count : (step + 1) * count].astype(F32)
    lane = lax.broadcasted_iota(jnp.int32, (count, RANK), 1).astype(F32)
    return jnp.where(rows == lane, 1.0, 0.0).astype(BF)


def picks(place, kept_ref, got_ref, step):
    half = kept_ref.shape[1] - RANK // 2
    mine = chosen(kept_ref[:, half : half + 1], step)
    theirs = chosen(got_ref[:, half : half + 1], step)
    first = place[0] == 0
    return jnp.concatenate(
        [jnp.where(first, mine, theirs), jnp.where(first, theirs, mine)], axis=0
    )


def own_half(place, x):
    half = x.shape[1] // 2
    return jnp.where(place[0] == 0, x[:, :half], x[:, half:])


def range_kernel(place, delta_hbm, part_ref, delta_ref, sem):
    rows, cols = delta_ref.shape
    split = rows // 2
    copies = [
        pltpu.make_async_copy(
            delta_hbm.at[pl.ds(i * split, split)], delta_ref.at[pl.ds(i * split, split)], sem.at[i]
        )
        for i in range(2)
    ]
    for copy in copies:
        copy.start()
    row_index = place[3] + lax.broadcasted_iota(jnp.int32, (cols, RANK), 0)
    col_index = lax.broadcasted_iota(jnp.int32, (cols, RANK), 1)
    hashed = row_index * RANK + col_index + place[4]
    hashed = hashed * 1103515245 + 12345
    hashed = hashed ^ lax.shift_right_logical(hashed, jnp.int32(16))
    hashed = hashed * 73244475
    hashed = hashed ^ lax.shift_right_logical(hashed, jnp.int32(15))
    parity = lax.shift_right_logical(hashed, jnp.int32(11)) & 1
    signs = (2 * parity - 1).astype(F32).astype(BF)
    parts = part_ref.shape[0] // 2
    for i, copy in enumerate(copies):
        copy.wait()
        product = dot(delta_ref[i * split : (i + 1) * split].astype(BF), signs)
        part_ref[i * parts : (i + 1) * parts] = product.astype(BF).reshape(
            parts, *part_ref.shape[1:]
        )


def pool_kernel(
    place, up_hbm, delta_ref, tokens_ref, pool_ref, gain_ref, gained_ref, up_out_ref, squares_ref, kept_ref, sent_ref, up_ref, sem
):
    core = place[0]
    z_half = place[1]
    width = up_ref.shape[0]
    first = pl.multiple_of(z_half * width, width)
    copy = pltpu.make_async_copy(up_hbm.at[pl.ds(first, width)], up_ref, sem.at[0])
    copy.start()
    delta = delta_ref[...].astype(BF)
    half = delta.shape[1] // 2
    left, right = delta[:, :half], delta[:, half:]
    tokens = jnp.concatenate([column(tokens_ref[i : i + 1].astype(F32)) for i in range(2)], axis=0)
    tokens = tokens[:, : RANK // 2].astype(BF)
    kept_ref[...] = jnp.concatenate([jnp.where(core == 0, left, right), tokens], axis=1)
    sent_ref[...] = jnp.concatenate([jnp.where(core == 0, right, left), tokens], axis=1)
    pool = jnp.where(z_half == 0, pool_ref[:, :width], pool_ref[:, width:]).astype(F32)
    gain = jnp.where(z_half == 0, gain_ref[:, :width].astype(F32), gain_ref[:, width:].astype(F32))
    gained = (pool * gain).astype(BF)
    gained_ref[...] = gained
    squares = jnp.broadcast_to(jnp.sum(pool * pool, axis=1, keepdims=True), (pool.shape[0], RANK))
    hi, lo = hi_lo(squares)
    squares_ref[0] = hi.astype(BF)
    squares_ref[1] = lo.astype(BF)
    copy.wait()
    up_out_ref[...] = own_half(place, dot(gained, up_ref[...])).astype(BF)


def spread_kernel(place, parts_ref, out_ref):
    out_ref[...] = jnp.broadcast_to(total(parts_ref).astype(BF), out_ref.shape)


def moved_kernel(place, basis_ref, kept_ref, got_ref, pool_ref, up_ref, squares_ref, out_ref):
    core = place[0]
    rows, wide = kept_ref.shape
    half = wide - RANK // 2
    count = basis_ref.shape[0] // 2
    own = basis_ref[pl.ds(core * count, count)].reshape(rows, RANK)
    other = basis_ref[pl.ds((1 - core) * count, count)].reshape(rows, RANK)
    basis = basis_ref[...].reshape(2 * rows, RANK)

    def put(first, values):
        values = values.astype(BF)
        out_ref[:, :, first : first + values.shape[1]] = values.reshape(
            *out_ref.shape[:2], values.shape[1]
        )

    moved = dot_t(own, kept_ref[...]) + dot_t(other, got_ref[...])
    put(0, jnp.concatenate([moved[:, :half].astype(BF), up_ref[...]], axis=1))
    squares = squares_ref[0].astype(F32) + squares_ref[1].astype(F32)
    put(2 * half, packed(dot_t(basis, basis), squares, diagonal_offset(RANK, 0)))
    put(2 * half + RANK, dot(pool_ref[...], basis))


def share_kernel(place, parts_ref, out_ref):
    share = total(parts_ref)
    rows, width = share.shape
    first = width - 2 * RANK
    offset = diagonal_offset(rows, place[2] * rows)
    gram = share[:, first : first + RANK]
    gram = packed(gram, unpacked_squares(gram, offset), offset)
    share = jnp.concatenate([share[:, :first], gram, share[:, first + RANK :]], axis=1)
    out_ref[...] = jnp.broadcast_to(share.astype(BF), out_ref.shape)


def down_copy(place, down_hbm, down_ref, sem):
    half = down_ref.shape[0]
    first = pl.multiple_of(place[0] * half, RANK // 2)
    return pltpu.make_async_copy(down_hbm.at[pl.ds(first, half)], down_ref, sem.at[0])


def first_kernel(place, down_hbm, z_ref, step_ref, coef_ref, pre_ref, down_ref, sem):
    copy = down_copy(place, down_hbm, down_ref, sem)
    copy.start()
    half = coef_ref.shape[1]
    gathered = z_ref[...].reshape(RANK, z_ref.shape[2])
    gram = gathered[:, 2 * half : 2 * half + RANK].astype(F32)
    row = lax.broadcasted_iota(jnp.int32, (RANK, RANK), 0)
    col = lax.broadcasted_iota(jnp.int32, (RANK, RANK), 1)
    offset = (col - row) & (RANK - 1)
    squares = unpacked_squares(gram, offset)
    gram = jnp.where(offset <= RANK // 2, gram, gram.T)
    eye = jnp.where(row == col, 1.0, 0.0)
    on_diag = gram * eye
    scale_col = lax.rsqrt(jnp.sum(on_diag, axis=1, keepdims=True))
    scale_row = lax.rsqrt(jnp.sum(on_diag, axis=0, keepdims=True))
    unit = gram * scale_col * scale_row
    bound = jnp.max(jnp.sum(jnp.abs(unit), axis=1, keepdims=True), axis=0, keepdims=True)
    step = 2.0 / (1.0 + bound)
    start = step * (2.0 * eye - step * unit)

    def going(state):
        count, error, _ = state
        return jnp.logical_and(count < 40, error > 2e-4)

    def refine(state):
        count, _, inverse = state
        left = eye - precise(unit, inverse)
        moved = dot(inverse.astype(BF), left.astype(BF))
        return count + 1, jnp.sum(left * left), inverse + moved

    _, _, inverse = lax.while_loop(going, refine, (0, jnp.float32(1.0), start))
    hi, lo = hi_lo(inverse * scale_col * scale_row)
    moved = gathered[:, :half]
    coef = (dot(hi.astype(BF), moved) + dot(lo.astype(BF), moved)).astype(BF)
    coef_ref[...] = coef
    pre = gathered[:, half : 2 * half].astype(F32) + dot(gathered[:, 2 * half + RANK :], coef)
    pre_ref[...] = pre.astype(BF)
    hidden = silu(pre * lax.rsqrt(squares / D + EPS)).astype(BF)
    copy.wait()
    result = dot(hidden, down_ref[...]).astype(BF)
    count, rows, width = step_ref.shape
    step_ref[: count // 2] = result[:, :width].reshape(count // 2, rows, width)
    step_ref[count // 2 :] = result[:, width:].reshape(count // 2, rows, width)


def second_kernel(
    place, up_hbm, step_ref, pool_ref, gain_ref, basis_ref, coef_ref, kept_ref, got_ref, out_ref, rows_ref, up_ref, sem
):
    z_half = place[1]
    _, _, width = step_ref.shape
    pool_rows = pool_ref.shape[0]
    start = pl.multiple_of(z_half * width, width)
    copy = pltpu.make_async_copy(up_hbm.at[pl.ds(start, width)], up_ref, sem.at[0])
    copy.start()
    half = coef_ref.shape[1]
    basis = basis_ref[...].reshape(width, RANK)
    step = step_ref[...].astype(F32).reshape(2, pool_rows, width)
    pool = pool_ref[...]
    left = (pool[:, :width].astype(F32) + step[0]).astype(BF)
    right = (pool[:, width:].astype(F32) + step[1]).astype(BF)
    carried = jnp.concatenate([left, right], axis=1)
    gain = jnp.where(z_half == 0, gain_ref[:, :width].astype(F32), gain_ref[:, width:].astype(F32))
    gained = (jnp.where(z_half == 0, left, right).astype(F32) * gain).astype(BF)

    def second(one, two):
        return (dot(one, carried) + dot(two, pool)).astype(BF)

    wide = second(
        picks(place, kept_ref, got_ref, 0), picks(place, kept_ref, got_ref, 1)
    ).astype(F32)
    squares = jnp.sum(wide * wide, axis=1, keepdims=True)
    row = lax.broadcasted_iota(jnp.int32, (rows_ref.shape[0], pool_rows), 0)
    lane = lax.broadcasted_iota(jnp.int32, (rows_ref.shape[0], pool_rows), 1)
    here = jnp.where(lane == row + place[5], 1.0, 0.0).astype(BF)
    tokens = kept_ref[:, half : half + 1]
    rows_ref[...] = second(
        dot(here, chosen(tokens, 0)).astype(BF), dot(here, chosen(tokens, 1)).astype(BF)
    )
    lane = lax.broadcasted_iota(jnp.int32, (pool_rows, out_ref.shape[2] - half), 1)
    first = 4 * z_half
    tail = jnp.zeros(lane.shape, F32)
    for place_in, value in enumerate((*hi_lo(squares[:pool_rows]), *hi_lo(squares[pool_rows:]))):
        tail = jnp.where(lane == first + place_in, value, tail)
    low = dot(dot(gained, basis).astype(BF), coef_ref[...])
    copy.wait()
    up = own_half(place, dot(gained, up_ref[...])) + low
    both = jnp.concatenate([up.astype(BF), tail.astype(BF)], axis=1)
    out_ref[...] = both.reshape(out_ref.shape)


def second_share_kernel(half, place, parts_ref, out_ref):
    share = total(parts_ref)
    lane = lax.broadcasted_iota(jnp.int32, share.shape, 1)
    out = share
    for first in range(half, half + 8, 2):
        whole = jnp.where(jnp.logical_or(lane == first, lane == first + 1), share, 0.0)
        hi, lo = hi_lo(jnp.sum(whole, axis=1, keepdims=True))
        out = jnp.where(lane == first, hi, jnp.where(lane == first + 1, lo, out))
    out_ref[...] = jnp.broadcast_to(out.astype(BF), out_ref.shape)


def last_kernel(place, down_hbm, z_ref, pre_ref, kept_ref, got_ref, out_ref, down_ref, sem):
    copy = down_copy(place, down_hbm, down_ref, sem)
    copy.start()
    z_half = place[1]
    half = pre_ref.shape[1]
    pool_rows = pre_ref.shape[0]
    gathered = z_ref[...].reshape(pool_rows, z_ref.shape[2])
    lane = lax.broadcasted_iota(jnp.int32, gathered.shape, 1)

    def squares(first):
        first = half + 4 * z_half + first
        chosen = jnp.logical_or(lane == first, lane == first + 1)
        return jnp.sum(jnp.where(chosen, gathered.astype(F32), 0.0), axis=1, keepdims=True)

    scale = lax.rsqrt(jnp.concatenate([squares(0), squares(2)], axis=0) / D + EPS)
    one, two = picks(place, kept_ref, got_ref, 0), picks(place, kept_ref, got_ref, 1)
    pre = dot(one, gathered[:, :half]) + dot(two, pre_ref[...])
    hidden = silu(pre * scale).astype(BF)
    copy.wait()
    out_ref[...] = dot(hidden, down_ref[...]).astype(BF).reshape(out_ref.shape)


def staged(weight_delta, sketch_seed, up_weight, down_weight, norm_gain, state_pool, token_rows):
    learner = lax.axis_index(L)
    rows, cols = weight_delta.shape
    half = cols // 2
    width = 2 * rows
    count = state_pool.shape[0]
    out_rows = count // 16
    place = jnp.stack(
        [
            lax.axis_index("c"),
            lax.axis_index("zh"),
            lax.axis_index(Z),
            learner * cols,
            sketch_seed[0] * 7919,
            learner * out_rows,
        ]
    ).astype(jnp.int32)
    padded = half + RANK // 2
    (part,) = call(
        range_kernel,
        ((16, rows // 16, RANK),),
        place,
        hbm=weight_delta,
        scratch=(pltpu.VMEM((rows, cols), F32),),
        limit=63.5,
    )
    parts = swap(part, L)
    gain = norm_gain[None]
    up_scratch = (pltpu.VMEM((width, cols), BF),)
    down_scratch = (pltpu.VMEM((half, 2 * width), BF),)
    gained, pool_up, squares, kept, sent = call(
        pool_kernel,
        ((count, width), (count, half), (2, count, RANK), (rows, padded), (rows, padded)),
        place, weight_delta, token_rows[:, 0, :], state_pool, gain,
        hbm=up_weight, scratch=up_scratch, limit=16,
    )
    received = lax.ppermute(sent, "c", [(0, 1), (1, 0)])
    parts, received, gained, pool_up, squares, kept, place, gain, pool = lax.optimization_barrier(
        (parts, received, gained, pool_up, squares, kept, place, gain, state_pool)
    )
    (spread,) = call(spread_kernel, ((32, rows // 16, RANK),), place, parts)
    basis = swap(spread, CL)
    (stacked,) = call(
        moved_kernel,
        ((16, count // 16, 2 * half + 2 * RANK),),
        place, basis, kept, received, gained, pool_up, squares,
    )
    (share,) = call(share_kernel, (stacked.shape,), place, swap(stacked, Z))
    step_part, coef, pool_pre = call(
        first_kernel,
        ((32, count // 16, width), (RANK, half), (count, half)),
        place, swap(share, Z),
        hbm=down_weight, scratch=down_scratch,
    )
    (spread,) = call(spread_kernel, (step_part.shape,), place, swap(step_part, CL))
    step = swap(spread, CL)
    stacked, own_second = call(
        second_kernel,
        ((16, count // 16, padded), (out_rows, 2 * width)),
        place, step, pool, gain, basis, coef, kept, received,
        hbm=up_weight, scratch=up_scratch,
    )
    (share,) = call(
        functools.partial(second_share_kernel, half), (stacked.shape,), place, swap(stacked, Z)
    )
    (last,) = call(
        last_kernel,
        ((32, out_rows, 2 * width),),
        place, swap(share, Z), pool_pre, kept, received,
        hbm=down_weight, scratch=down_scratch,
    )
    last_share = jnp.sum(swap(last, CL).astype(F32), axis=0)
    return (own_second.astype(F32) + last_share).astype(BF)[None]


def solution(mesh):
    torus = Mesh(
        mesh.devices.reshape(4, 4, mesh.shape["rollout"], 2, 2), ("y", "x", "zl", "zh", "c")
    )
    return jax.shard_map(
        staged,
        mesh=torus,
        in_specs=(
            P(("zl", "zh", "c"), L),
            P(),
            P("zl", L),
            P(L, "zl"),
            P("zl"),
            P(None, "zl"),
            P(None, ("zh", "c"), None),
        ),
        out_specs=P(("zh", "c"), L, "zl"),
        check_vma=False,
    )
```

```python
import functools

import jax
import jax.numpy as jnp
from jax import lax
from jax.experimental import pallas as pl
from jax.experimental.pallas import tpu as pltpu
from jax.sharding import Mesh
from jax.sharding import PartitionSpec as P


D = 8192
RANK = 128
EPS = 1e-05
L = ("y", "x")
CL = ("c", "y", "x")
Z = ("zl", "zh")
BF = jnp.bfloat16
F32 = jnp.float32


def swap(x, axis):
    return lax.all_to_all(x, axis, split_axis=0, concat_axis=0, tiled=True)


def dot(a, b):
    return jnp.dot(a, b, preferred_element_type=F32)


def dot_t(a, b):
    return lax.dot_general(a, b, (((0,), (0,)), ((), ())), preferred_element_type=F32)


def hi_lo(x):
    hi = x.astype(BF).astype(F32)
    return hi, x - hi


def diagonal_offset(rows, first):
    row = first + lax.broadcasted_iota(jnp.int32, (rows, RANK), 0)
    col = lax.broadcasted_iota(jnp.int32, (rows, RANK), 1)
    return (col - row) & (RANK - 1)


def packed(gram, squares, offset):
    hi, lo = hi_lo(squares)
    rest = jnp.where(offset == RANK - 1, lo, jnp.where(offset == RANK - 2, hi, 0.0))
    return jnp.where(offset <= RANK // 2, gram, rest)


def unpacked_squares(gram, offset):
    return jnp.sum(jnp.where(offset >= RANK - 2, gram, 0.0), axis=1, keepdims=True)


def precise(a, b):
    return jnp.dot(a, b, precision=lax.Precision.HIGHEST, preferred_element_type=F32)


def silu(x):
    return x / (1.0 + jnp.exp(-x))


def total(ref):
    return jnp.sum(ref[...].astype(F32), axis=0)


HBM = pl.BlockSpec(memory_space=pltpu.HBM)
VMEM = pl.BlockSpec(memory_space=pltpu.VMEM)


def call(kernel, shapes, place, *arrays, hbm=None, scratch=()):
    specs = [pl.BlockSpec(memory_space=pltpu.SMEM)]
    if hbm is not None:
        arrays = (hbm, *arrays)
        specs += [HBM]
        scratch = (*scratch, pltpu.SemaphoreType.DMA((2,)))
    specs += [VMEM] * (len(arrays) - (hbm is not None))
    return pl.pallas_call(
        kernel,
        out_shape=tuple(jax.ShapeDtypeStruct(shape, BF) for shape in shapes),
        in_specs=specs,
        out_specs=(VMEM,) * len(shapes),
        scratch_shapes=scratch,
        compiler_params=pltpu.CompilerParams(vmem_limit_bytes=16 * 1024 * 1024),
    )(place, *arrays)


def column(row):
    return jnp.broadcast_to(row, (RANK, RANK)).T


def chosen(tokens, step):
    count = tokens.shape[0] // 2
    rows = tokens[step * count : (step + 1) * count].astype(F32)
    lane = lax.broadcasted_iota(jnp.int32, (count, RANK), 1).astype(F32)
    return jnp.where(rows == lane, 1.0, 0.0).astype(BF)


def picks(place, kept_ref, got_ref, step):
    half = kept_ref.shape[1] - RANK // 2
    mine = chosen(kept_ref[:, half : half + 1], step)
    theirs = chosen(got_ref[:, half : half + 1], step)
    first = place[0] == 0
    return jnp.concatenate(
        [jnp.where(first, mine, theirs), jnp.where(first, theirs, mine)], axis=0
    )


def own_half(place, x):
    half = x.shape[1] // 2
    return jnp.where(place[0] == 0, x[:, :half], x[:, half:])


def range_kernel(place, delta_hbm, tokens_ref, part_ref, kept_ref, sent_ref, delta_ref, sem):
    core = place[0]
    rows, cols = delta_ref.shape
    half = cols // 2
    split = rows // 2
    copies = [
        pltpu.make_async_copy(
            delta_hbm.at[pl.ds(i * split, split)], delta_ref.at[pl.ds(i * split, split)], sem.at[i]
        )
        for i in range(2)
    ]
    for copy in copies:
        copy.start()
    row_index = place[3] + lax.broadcasted_iota(jnp.int32, (cols, RANK), 0)
    col_index = lax.broadcasted_iota(jnp.int32, (cols, RANK), 1)
    hashed = row_index * RANK + col_index + place[4]
    hashed = hashed * 1103515245 + 12345
    hashed = hashed ^ lax.shift_right_logical(hashed, jnp.int32(16))
    hashed = hashed * 73244475
    hashed = hashed ^ lax.shift_right_logical(hashed, jnp.int32(15))
    parity = lax.shift_right_logical(hashed, jnp.int32(11)) & 1
    signs = (2 * parity - 1).astype(F32).astype(BF)
    for i, copy in enumerate(copies):
        copy.wait()
        span = slice(i * split, (i + 1) * split)
        delta = delta_ref[span].astype(BF)
        parts = part_ref.shape[0] // 2
        part_ref[i * parts : (i + 1) * parts] = (
            dot(delta, signs).astype(BF).reshape(parts, *part_ref.shape[1:])
        )
        left, right = delta[:, :half], delta[:, half:]
        tokens = column(tokens_ref[i : i + 1].astype(F32))[:, : RANK // 2].astype(BF)
        kept_ref[span] = jnp.concatenate([jnp.where(core == 0, left, right), tokens], axis=1)
        sent_ref[span] = jnp.concatenate([jnp.where(core == 0, right, left), tokens], axis=1)


def pool_kernel(place, up_hbm, pool_ref, gain_ref, gained_ref, up_out_ref, squares_ref, up_ref, sem):
    z_half = place[1]
    width = up_ref.shape[0]
    first = pl.multiple_of(z_half * width, width)
    copy = pltpu.make_async_copy(up_hbm.at[pl.ds(first, width)], up_ref, sem.at[0])
    copy.start()
    pool = jnp.where(z_half == 0, pool_ref[:, :width], pool_ref[:, width:]).astype(F32)
    gain = jnp.where(z_half == 0, gain_ref[:, :width], gain_ref[:, width:])
    gained = (pool * gain).astype(BF)
    gained_ref[...] = gained
    squares = jnp.broadcast_to(jnp.sum(pool * pool, axis=1, keepdims=True), (pool.shape[0], RANK))
    hi, lo = hi_lo(squares)
    squares_ref[0] = hi.astype(BF)
    squares_ref[1] = lo.astype(BF)
    copy.wait()
    up_out_ref[...] = own_half(place, dot(gained, up_ref[...])).astype(BF)


def spread_kernel(place, parts_ref, out_ref, share_ref):
    share = total(parts_ref).astype(BF)
    share_ref[...] = share
    out_ref[...] = jnp.broadcast_to(share, out_ref.shape)


def step_spread_kernel(place, parts_ref, basis_ref, out_ref):
    rows = out_ref.shape[1]
    basis = basis_ref[...].astype(F32)
    share = jnp.concatenate([total(parts_ref), basis[:rows], basis[rows:]], axis=1)
    out_ref[...] = jnp.broadcast_to(share.astype(BF), out_ref.shape)


def moved_kernel(place, basis_ref, kept_ref, got_ref, pool_ref, up_ref, squares_ref, out_ref):
    core = place[0]
    rows, wide = kept_ref.shape
    half = wide - RANK // 2
    count = basis_ref.shape[0] // 2
    own = basis_ref[pl.ds(core * count, count)].reshape(rows, RANK)
    other = basis_ref[pl.ds((1 - core) * count, count)].reshape(rows, RANK)
    basis = basis_ref[...].reshape(2 * rows, RANK)

    def put(first, values):
        values = values.astype(BF)
        out_ref[:, :, first : first + values.shape[1]] = values.reshape(
            *out_ref.shape[:2], values.shape[1]
        )

    moved = dot_t(own, kept_ref[...]) + dot_t(other, got_ref[...])
    put(0, jnp.concatenate([moved[:, :half].astype(BF), up_ref[...]], axis=1))
    squares = squares_ref[0].astype(F32) + squares_ref[1].astype(F32)
    put(2 * half, packed(dot_t(basis, basis), squares, diagonal_offset(RANK, 0)))
    put(2 * half + RANK, dot(pool_ref[...], basis))


def share_kernel(place, parts_ref, out_ref):
    share = total(parts_ref)
    rows, width = share.shape
    first = width - 2 * RANK
    offset = diagonal_offset(rows, place[2] * rows)
    gram = share[:, first : first + RANK]
    gram = packed(gram, unpacked_squares(gram, offset), offset)
    share = jnp.concatenate([share[:, :first], gram, share[:, first + RANK :]], axis=1)
    out_ref[...] = jnp.broadcast_to(share.astype(BF), out_ref.shape)


def down_copy(place, down_hbm, down_ref, sem):
    half = down_ref.shape[0]
    first = pl.multiple_of(place[0] * half, RANK // 2)
    return pltpu.make_async_copy(down_hbm.at[pl.ds(first, half)], down_ref, sem.at[0])


def first_kernel(place, down_hbm, z_ref, step_ref, coef_ref, pre_ref, down_ref, sem):
    copy = down_copy(place, down_hbm, down_ref, sem)
    copy.start()
    half = coef_ref.shape[1]
    gathered = z_ref[...].reshape(RANK, z_ref.shape[2])
    gram = gathered[:, 2 * half : 2 * half + RANK].astype(F32)
    row = lax.broadcasted_iota(jnp.int32, (RANK, RANK), 0)
    col = lax.broadcasted_iota(jnp.int32, (RANK, RANK), 1)
    offset = (col - row) & (RANK - 1)
    squares = unpacked_squares(gram, offset)
    gram = jnp.where(offset <= RANK // 2, gram, gram.T)
    eye = jnp.where(row == col, 1.0, 0.0)
    on_diag = gram * eye
    scale_col = lax.rsqrt(jnp.sum(on_diag, axis=1, keepdims=True))
    scale_row = lax.rsqrt(jnp.sum(on_diag, axis=0, keepdims=True))
    unit = gram * scale_col * scale_row
    bound = jnp.max(jnp.sum(jnp.abs(unit), axis=1, keepdims=True), axis=0, keepdims=True)
    step = 2.0 / (1.0 + bound)
    start = step * (2.0 * eye - step * unit)

    def going(state):
        count, error, _ = state
        return jnp.logical_and(count < 40, error > 2e-4)

    def refine(state):
        count, _, inverse = state
        left = eye - precise(unit, inverse)
        moved = dot(inverse.astype(BF), left.astype(BF))
        return count + 1, jnp.sum(left * left), inverse + moved

    _, _, inverse = lax.while_loop(going, refine, (0, jnp.float32(1.0), start))
    hi, lo = hi_lo(inverse * scale_col * scale_row)
    moved = gathered[:, :half]
    coef = (dot(hi.astype(BF), moved) + dot(lo.astype(BF), moved)).astype(BF)
    coef_ref[...] = coef
    pre = gathered[:, half : 2 * half].astype(F32) + dot(gathered[:, 2 * half + RANK :], coef)
    pre_ref[...] = pre.astype(BF)
    hidden = silu(pre * lax.rsqrt(squares / D + EPS)).astype(BF)
    copy.wait()
    result = dot(hidden, down_ref[...]).astype(BF)
    count, rows, width = step_ref.shape
    step_ref[: count // 2] = result[:, :width].reshape(count // 2, rows, width)
    step_ref[count // 2 :] = result[:, width:].reshape(count // 2, rows, width)


def second_kernel(
    place, step_ref, pool_ref, gain_ref, up_ref, basis_ref, coef_ref, kept_ref, got_ref, out_ref, rows_ref
):
    z_half = place[1]
    pool_rows = pool_ref.shape[0]
    half = coef_ref.shape[1]
    basis = basis_ref[...].reshape(-1, RANK)
    width = basis.shape[0]
    wide = step_ref[...].astype(F32)
    other = jnp.concatenate(
        [wide[:, :, width : width + RANK], wide[:, :, width + RANK :]], axis=1
    ).reshape(width, RANK).astype(BF)
    step = wide[:, :, :width].reshape(2, pool_rows, width)
    pool = pool_ref[...]
    left = (pool[:, :width].astype(F32) + step[0]).astype(BF)
    right = (pool[:, width:].astype(F32) + step[1]).astype(BF)
    carried = jnp.concatenate([left, right], axis=1)
    gained_left = (left.astype(F32) * gain_ref[:, :width]).astype(BF)
    gained_right = (right.astype(F32) * gain_ref[:, width:]).astype(BF)
    gained = jnp.concatenate([gained_left, gained_right], axis=1)
    gained_own = jnp.where(z_half == 0, gained_left, gained_right)
    gained_other = jnp.where(z_half == 0, gained_right, gained_left)

    def second(one, two):
        return (dot(one, carried) + dot(two, pool)).astype(BF)

    wide = second(
        picks(place, kept_ref, got_ref, 0), picks(place, kept_ref, got_ref, 1)
    ).astype(F32)
    squares = jnp.sum(wide * wide, axis=1, keepdims=True)
    row = lax.broadcasted_iota(jnp.int32, (rows_ref.shape[0], pool_rows), 0)
    lane = lax.broadcasted_iota(jnp.int32, (rows_ref.shape[0], pool_rows), 1)
    here = jnp.where(lane == row + place[5], 1.0, 0.0).astype(BF)
    tokens = kept_ref[:, half : half + 1]
    rows_ref[...] = second(
        dot(here, chosen(tokens, 0)).astype(BF), dot(here, chosen(tokens, 1)).astype(BF)
    )
    lane = lax.broadcasted_iota(jnp.int32, (pool_rows, RANK // 2), 1)
    tail = jnp.zeros(lane.shape, F32)
    for place_in, value in enumerate((*hi_lo(squares[:pool_rows]), *hi_lo(squares[pool_rows:]))):
        tail = jnp.where(lane == place_in, value, tail)
    low = dot(gained_own, basis) + dot(gained_other, other)
    up = own_half(place, dot(gained, up_ref[...])) + dot(low.astype(BF), coef_ref[...])
    both = jnp.concatenate([up.astype(BF), tail.astype(BF)], axis=1)
    out_ref[...] = both.reshape(out_ref.shape)


def second_share_kernel(half, place, parts_ref, out_ref):
    share = total(parts_ref)
    lane = lax.broadcasted_iota(jnp.int32, share.shape, 1)
    out = share
    for first in range(half, half + 4, 2):
        whole = jnp.where(jnp.logical_or(lane == first, lane == first + 1), share, 0.0)
        hi, lo = hi_lo(jnp.sum(whole, axis=1, keepdims=True))
        out = jnp.where(lane == first, hi, jnp.where(lane == first + 1, lo, out))
    out_ref[...] = jnp.broadcast_to(out.astype(BF), out_ref.shape)


def last_kernel(place, down_hbm, z_ref, pre_ref, kept_ref, got_ref, out_ref, down_ref, sem):
    copy = down_copy(place, down_hbm, down_ref, sem)
    copy.start()
    half = pre_ref.shape[1]
    pool_rows = pre_ref.shape[0]
    gathered = z_ref[...].reshape(pool_rows, z_ref.shape[2])
    lane = lax.broadcasted_iota(jnp.int32, gathered.shape, 1)

    def squares(first):
        first = half + first
        chosen = jnp.logical_or(lane == first, lane == first + 1)
        return jnp.sum(jnp.where(chosen, gathered.astype(F32), 0.0), axis=1, keepdims=True)

    scale = lax.rsqrt(jnp.concatenate([squares(0), squares(2)], axis=0) / D + EPS)
    one, two = picks(place, kept_ref, got_ref, 0), picks(place, kept_ref, got_ref, 1)
    pre = dot(one, gathered[:, :half]) + dot(two, pre_ref[...])
    hidden = silu(pre * scale).astype(BF)
    copy.wait()
    out_ref[...] = dot(hidden, down_ref[...]).astype(BF).reshape(out_ref.shape)


def staged(weight_delta, sketch_seed, up_weight, down_weight, norm_gain, state_pool, token_rows):
    learner = lax.axis_index(L)
    rows, cols = weight_delta.shape
    half = cols // 2
    width = 2 * rows
    count = state_pool.shape[0]
    out_rows = count // 16
    place = jnp.stack(
        [
            lax.axis_index("c"),
            lax.axis_index("zh"),
            lax.axis_index(Z),
            learner * cols,
            sketch_seed[0] * 7919,
            learner * out_rows,
        ]
    ).astype(jnp.int32)
    padded = half + RANK // 2
    part, kept, sent = call(
        range_kernel,
        ((16, rows // 16, RANK), (rows, padded), (rows, padded)),
        place,
        token_rows[:, 0, :],
        hbm=weight_delta,
        scratch=(pltpu.VMEM((rows, cols), F32),),
    )
    received = lax.ppermute(sent, "c", [(0, 1), (1, 0)])
    parts = swap(part, L)
    gain = norm_gain.astype(F32)[None]
    up_scratch = (pltpu.VMEM((width, cols), BF),)
    down_scratch = (pltpu.VMEM((half, 2 * width), BF),)
    parts, received, kept, place, gain, pool = lax.optimization_barrier(
        (parts, received, kept, place, gain, state_pool)
    )
    spread, range_share = call(
        spread_kernel, ((32, rows // 16, RANK), (rows // 16, RANK)), place, parts
    )
    other_share = lax.ppermute(range_share, "zh", [(0, 1), (1, 0)])
    basis = swap(spread, CL)
    gained, pool_up, squares = call(
        pool_kernel,
        ((count, width), (count, half), (2, count, RANK)),
        place, pool, gain,
        hbm=up_weight, scratch=up_scratch,
    )
    (stacked,) = call(
        moved_kernel,
        ((16, count // 16, 2 * half + 2 * RANK),),
        place, basis, kept, received, gained, pool_up, squares,
    )
    (share,) = call(share_kernel, (stacked.shape,), place, swap(stacked, Z))
    step_part, coef, pool_pre = call(
        first_kernel,
        ((32, count // 16, width), (RANK, half), (count, half)),
        place, swap(share, Z),
        hbm=down_weight, scratch=down_scratch,
    )
    (spread,) = call(
        step_spread_kernel,
        ((*step_part.shape[:2], width + 2 * RANK),),
        place, swap(step_part, CL), other_share,
    )
    step = swap(spread, CL)
    stacked, own_second = call(
        second_kernel,
        ((8, count // 8, padded), (out_rows, 2 * width)),
        place, step, pool, gain, up_weight, basis, coef, kept, received,
    )
    (share,) = call(
        functools.partial(second_share_kernel, half), (stacked.shape,), place, swap(stacked, "zl")
    )
    (last,) = call(
        last_kernel,
        ((32, out_rows, 2 * width),),
        place, swap(share, "zl"), pool_pre, kept, received,
        hbm=down_weight, scratch=down_scratch,
    )
    last_share = jnp.sum(swap(last, CL).astype(F32), axis=0)
    return (own_second.astype(F32) + last_share).astype(BF)[None]


def solution(mesh):
    torus = Mesh(
        mesh.devices.reshape(4, 4, mesh.shape["rollout"], 2, 2), ("y", "x", "zl", "zh", "c")
    )
    return jax.shard_map(
        staged,
        mesh=torus,
        in_specs=(
            P(("zl", "zh", "c"), L),
            P(),
            P("zl", L),
            P(L, "zl"),
            P("zl"),
            P(None, "zl"),
            P(None, ("zh", "c"), None),
        ),
        out_specs=P(("zh", "c"), L, "zl"),
        check_vma=False,
    )
```

```python
import functools

import jax
import jax.numpy as jnp
from jax import lax
from jax.experimental import pallas as pl
from jax.experimental.pallas import tpu as pltpu
from jax.sharding import Mesh
from jax.sharding import PartitionSpec as P


D = 8192
RANK = 128
EPS = 1e-05
L = ("y", "x")
CL = ("c", "y", "x")
Z = ("zl", "zh")
BF = jnp.bfloat16
F32 = jnp.float32


def swap(x, axis):
    return lax.all_to_all(x, axis, split_axis=0, concat_axis=0, tiled=True)


def dot(a, b):
    return jnp.dot(a, b, preferred_element_type=F32)


def dot_t(a, b):
    return lax.dot_general(a, b, (((0,), (0,)), ((), ())), preferred_element_type=F32)


def hi_lo(x):
    hi = x.astype(BF).astype(F32)
    return hi, x - hi


def diagonal_offset(rows, first):
    row = first + lax.broadcasted_iota(jnp.int32, (rows, RANK), 0)
    col = lax.broadcasted_iota(jnp.int32, (rows, RANK), 1)
    return (col - row) & (RANK - 1)


def packed(gram, squares, offset):
    hi, lo = hi_lo(squares)
    rest = jnp.where(offset == RANK - 1, lo, jnp.where(offset == RANK - 2, hi, 0.0))
    return jnp.where(offset <= RANK // 2, gram, rest)


def unpacked_squares(gram, offset):
    return jnp.sum(jnp.where(offset >= RANK - 2, gram, 0.0), axis=1, keepdims=True)


def precise(a, b):
    return jnp.dot(a, b, precision=lax.Precision.HIGHEST, preferred_element_type=F32)


def silu(x):
    return x / (1.0 + jnp.exp(-x))


def total(ref):
    return jnp.sum(ref[...].astype(F32), axis=0)


HBM = pl.BlockSpec(memory_space=pltpu.HBM)
VMEM = pl.BlockSpec(memory_space=pltpu.VMEM)


def call(kernel, shapes, place, *arrays, hbm=None, scratch=()):
    specs = [pl.BlockSpec(memory_space=pltpu.SMEM)]
    if hbm is not None:
        arrays = (hbm, *arrays)
        specs += [HBM]
        scratch = (*scratch, pltpu.SemaphoreType.DMA((2,)))
    specs += [VMEM] * (len(arrays) - (hbm is not None))
    return pl.pallas_call(
        kernel,
        out_shape=tuple(jax.ShapeDtypeStruct(shape, BF) for shape in shapes),
        in_specs=specs,
        out_specs=(VMEM,) * len(shapes),
        scratch_shapes=scratch,
        compiler_params=pltpu.CompilerParams(vmem_limit_bytes=16 * 1024 * 1024),
    )(place, *arrays)


def column(row):
    return jnp.broadcast_to(row, (RANK, RANK)).T


def chosen(tokens, step):
    count = tokens.shape[0] // 2
    rows = tokens[step * count : (step + 1) * count].astype(F32)
    lane = lax.broadcasted_iota(jnp.int32, (count, RANK), 1).astype(F32)
    return jnp.where(rows == lane, 1.0, 0.0).astype(BF)


def picks(place, kept_ref, got_ref, step):
    half = kept_ref.shape[1] - RANK // 2
    mine = chosen(kept_ref[:, half : half + 1], step)
    theirs = chosen(got_ref[:, half : half + 1], step)
    first = place[0] == 0
    return jnp.concatenate(
        [jnp.where(first, mine, theirs), jnp.where(first, theirs, mine)], axis=0
    )


def own_half(place, x):
    half = x.shape[1] // 2
    return jnp.where(place[0] == 0, x[:, :half], x[:, half:])


def range_kernel(place, delta_hbm, tokens_ref, part_ref, kept_ref, sent_ref, delta_ref, sem):
    core = place[0]
    rows, cols = delta_ref.shape
    half = cols // 2
    split = rows // 2
    copies = [
        pltpu.make_async_copy(
            delta_hbm.at[pl.ds(i * split, split)], delta_ref.at[pl.ds(i * split, split)], sem.at[i]
        )
        for i in range(2)
    ]
    for copy in copies:
        copy.start()
    row_index = place[3] + lax.broadcasted_iota(jnp.int32, (cols, RANK), 0)
    col_index = lax.broadcasted_iota(jnp.int32, (cols, RANK), 1)
    hashed = row_index * RANK + col_index + place[4]
    hashed = hashed * 1103515245 + 12345
    hashed = hashed ^ lax.shift_right_logical(hashed, jnp.int32(16))
    hashed = hashed * 73244475
    hashed = hashed ^ lax.shift_right_logical(hashed, jnp.int32(15))
    parity = lax.shift_right_logical(hashed, jnp.int32(11)) & 1
    signs = (2 * parity - 1).astype(F32).astype(BF)
    for i, copy in enumerate(copies):
        copy.wait()
        span = slice(i * split, (i + 1) * split)
        delta = delta_ref[span].astype(BF)
        parts = part_ref.shape[0] // 2
        part_ref[i * parts : (i + 1) * parts] = (
            dot(delta, signs).astype(BF).reshape(parts, *part_ref.shape[1:])
        )
        left, right = delta[:, :half], delta[:, half:]
        tokens = column(tokens_ref[i : i + 1].astype(F32))[:, : RANK // 2].astype(BF)
        kept_ref[span] = jnp.concatenate([jnp.where(core == 0, left, right), tokens], axis=1)
        sent_ref[span] = jnp.concatenate([jnp.where(core == 0, right, left), tokens], axis=1)


def pick_kernel(place, kept_ref, got_ref, pick_ref):
    for step in range(2):
        pick_ref[step] = picks(place, kept_ref, got_ref, step)


def pool_kernel(place, up_hbm, pool_ref, gain_ref, gained_ref, up_out_ref, squares_ref, up_ref, sem):
    z_half = place[1]
    width = up_ref.shape[0]
    first = pl.multiple_of(z_half * width, width)
    copy = pltpu.make_async_copy(up_hbm.at[pl.ds(first, width)], up_ref, sem.at[0])
    copy.start()
    pool = jnp.where(z_half == 0, pool_ref[:, :width], pool_ref[:, width:]).astype(F32)
    gain = jnp.where(z_half == 0, gain_ref[:, :width], gain_ref[:, width:])
    gained = (pool * gain).astype(BF)
    gained_ref[...] = gained
    squares = jnp.broadcast_to(jnp.sum(pool * pool, axis=1, keepdims=True), (pool.shape[0], RANK))
    hi, lo = hi_lo(squares)
    squares_ref[0] = hi.astype(BF)
    squares_ref[1] = lo.astype(BF)
    copy.wait()
    up_out_ref[...] = own_half(place, dot(gained, up_ref[...])).astype(BF)


def spread_kernel(place, parts_ref, out_ref, share_ref):
    share = total(parts_ref).astype(BF)
    share_ref[...] = share
    out_ref[...] = jnp.broadcast_to(share, out_ref.shape)


def step_spread_kernel(place, parts_ref, basis_ref, out_ref):
    rows = out_ref.shape[1]
    basis = basis_ref[...].astype(F32)
    share = jnp.concatenate([total(parts_ref), basis[:rows], basis[rows:]], axis=1)
    out_ref[...] = jnp.broadcast_to(share.astype(BF), out_ref.shape)


def moved_kernel(place, basis_ref, kept_ref, got_ref, pool_ref, up_ref, squares_ref, out_ref):
    core = place[0]
    rows, wide = kept_ref.shape
    half = wide - RANK // 2
    count = basis_ref.shape[0] // 2
    own = basis_ref[pl.ds(core * count, count)].reshape(rows, RANK)
    other = basis_ref[pl.ds((1 - core) * count, count)].reshape(rows, RANK)
    basis = basis_ref[...].reshape(2 * rows, RANK)

    def put(first, values):
        values = values.astype(BF)
        out_ref[:, :, first : first + values.shape[1]] = values.reshape(
            *out_ref.shape[:2], values.shape[1]
        )

    moved = dot_t(own, kept_ref[...]) + dot_t(other, got_ref[...])
    put(0, jnp.concatenate([moved[:, :half].astype(BF), up_ref[...]], axis=1))
    squares = squares_ref[0].astype(F32) + squares_ref[1].astype(F32)
    put(2 * half, packed(dot_t(basis, basis), squares, diagonal_offset(RANK, 0)))
    put(2 * half + RANK, dot(pool_ref[...], basis))


def share_kernel(place, parts_ref, out_ref):
    share = total(parts_ref)
    rows, width = share.shape
    first = width - 2 * RANK
    offset = diagonal_offset(rows, place[2] * rows)
    gram = share[:, first : first + RANK]
    gram = packed(gram, unpacked_squares(gram, offset), offset)
    share = jnp.concatenate([share[:, :first], gram, share[:, first + RANK :]], axis=1)
    out_ref[...] = jnp.broadcast_to(share.astype(BF), out_ref.shape)


def down_copy(place, down_hbm, down_ref, sem):
    half = down_ref.shape[0]
    first = pl.multiple_of(place[0] * half, RANK // 2)
    return pltpu.make_async_copy(down_hbm.at[pl.ds(first, half)], down_ref, sem.at[0])


def first_kernel(place, down_hbm, z_ref, step_ref, coef_ref, pre_ref, down_ref, sem):
    copy = down_copy(place, down_hbm, down_ref, sem)
    copy.start()
    half = coef_ref.shape[1]
    gathered = z_ref[...].reshape(RANK, z_ref.shape[2])
    gram = gathered[:, 2 * half : 2 * half + RANK].astype(F32)
    row = lax.broadcasted_iota(jnp.int32, (RANK, RANK), 0)
    col = lax.broadcasted_iota(jnp.int32, (RANK, RANK), 1)
    offset = (col - row) & (RANK - 1)
    squares = unpacked_squares(gram, offset)
    gram = jnp.where(offset <= RANK // 2, gram, gram.T)
    eye = jnp.where(row == col, 1.0, 0.0)
    on_diag = gram * eye
    scale_col = lax.rsqrt(jnp.sum(on_diag, axis=1, keepdims=True))
    scale_row = lax.rsqrt(jnp.sum(on_diag, axis=0, keepdims=True))
    unit = gram * scale_col * scale_row
    bound = jnp.max(jnp.sum(jnp.abs(unit), axis=1, keepdims=True), axis=0, keepdims=True)
    step = 2.0 / (1.0 + bound)
    start = step * (2.0 * eye - step * unit)

    def going(state):
        count, error, _ = state
        return jnp.logical_and(count < 40, error > 2e-4)

    def refine(state):
        count, _, inverse = state
        left = eye - precise(unit, inverse)
        moved = dot(inverse.astype(BF), left.astype(BF))
        return count + 1, jnp.sum(left * left), inverse + moved

    _, _, inverse = lax.while_loop(going, refine, (0, jnp.float32(1.0), start))
    hi, lo = hi_lo(inverse * scale_col * scale_row)
    moved = gathered[:, :half]
    coef = (dot(hi.astype(BF), moved) + dot(lo.astype(BF), moved)).astype(BF)
    coef_ref[...] = coef
    pre = gathered[:, half : 2 * half].astype(F32) + dot(gathered[:, 2 * half + RANK :], coef)
    pre_ref[...] = pre.astype(BF)
    hidden = silu(pre * lax.rsqrt(squares / D + EPS)).astype(BF)
    copy.wait()
    result = dot(hidden, down_ref[...]).astype(BF)
    count, rows, width = step_ref.shape
    step_ref[: count // 2] = result[:, :width].reshape(count // 2, rows, width)
    step_ref[count // 2 :] = result[:, width:].reshape(count // 2, rows, width)


def second_kernel(
    place, step_ref, pool_ref, gain_ref, up_ref, basis_ref, coef_ref, pick_ref, out_ref, rows_ref
):
    z_half = place[1]
    pool_rows = pool_ref.shape[0]
    basis = basis_ref[...].reshape(-1, RANK)
    width = basis.shape[0]
    wide = step_ref[...].astype(F32)
    other = jnp.concatenate(
        [wide[:, :, width : width + RANK], wide[:, :, width + RANK :]], axis=1
    ).reshape(width, RANK).astype(BF)
    step = wide[:, :, :width].reshape(2, pool_rows, width)
    pool = pool_ref[...]
    left = (pool[:, :width].astype(F32) + step[0]).astype(BF)
    right = (pool[:, width:].astype(F32) + step[1]).astype(BF)
    carried = jnp.concatenate([left, right], axis=1)
    gained_left = (left.astype(F32) * gain_ref[:, :width]).astype(BF)
    gained_right = (right.astype(F32) * gain_ref[:, width:]).astype(BF)
    gained = jnp.concatenate([gained_left, gained_right], axis=1)
    gained_own = jnp.where(z_half == 0, gained_left, gained_right)
    gained_other = jnp.where(z_half == 0, gained_right, gained_left)

    def second(one, two):
        return (dot(one, carried) + dot(two, pool)).astype(BF)

    wide = second(pick_ref[0], pick_ref[1]).astype(F32)
    squares = jnp.sum(wide * wide, axis=1, keepdims=True)
    row = lax.broadcasted_iota(jnp.int32, (rows_ref.shape[0], pool_rows), 0)
    lane = lax.broadcasted_iota(jnp.int32, (rows_ref.shape[0], pool_rows), 1)
    here = jnp.where(lane == row + place[5], 1.0, 0.0).astype(BF)
    own = [
        dot(here, jnp.where(place[0] == 0, pick_ref[i, :pool_rows], pick_ref[i, pool_rows:]))
        for i in range(2)
    ]
    rows_ref[...] = second(own[0].astype(BF), own[1].astype(BF))
    lane = lax.broadcasted_iota(jnp.int32, (pool_rows, RANK // 2), 1)
    tail = jnp.zeros(lane.shape, F32)
    for place_in, value in enumerate((*hi_lo(squares[:pool_rows]), *hi_lo(squares[pool_rows:]))):
        tail = jnp.where(lane == place_in, value, tail)
    low = dot(gained_own, basis) + dot(gained_other, other)
    up = own_half(place, dot(gained, up_ref[...])) + dot(low.astype(BF), coef_ref[...])
    both = jnp.concatenate([up.astype(BF), tail.astype(BF)], axis=1)
    out_ref[...] = both.reshape(out_ref.shape)


def second_share_kernel(half, place, parts_ref, out_ref):
    share = total(parts_ref)
    lane = lax.broadcasted_iota(jnp.int32, share.shape, 1)
    out = share
    for first in range(half, half + 4, 2):
        whole = jnp.where(jnp.logical_or(lane == first, lane == first + 1), share, 0.0)
        hi, lo = hi_lo(jnp.sum(whole, axis=1, keepdims=True))
        out = jnp.where(lane == first, hi, jnp.where(lane == first + 1, lo, out))
    out_ref[...] = jnp.broadcast_to(out.astype(BF), out_ref.shape)


def last_kernel(place, down_hbm, z_ref, pre_ref, pick_ref, out_ref, down_ref, sem):
    copy = down_copy(place, down_hbm, down_ref, sem)
    copy.start()
    half = pre_ref.shape[1]
    pool_rows = pre_ref.shape[0]
    gathered = z_ref[...].reshape(pool_rows, z_ref.shape[2])
    lane = lax.broadcasted_iota(jnp.int32, gathered.shape, 1)

    def squares(first):
        first = half + first
        chosen = jnp.logical_or(lane == first, lane == first + 1)
        return jnp.sum(jnp.where(chosen, gathered.astype(F32), 0.0), axis=1, keepdims=True)

    scale = lax.rsqrt(jnp.concatenate([squares(0), squares(2)], axis=0) / D + EPS)
    pre = dot(pick_ref[0], gathered[:, :half]) + dot(pick_ref[1], pre_ref[...])
    hidden = silu(pre * scale).astype(BF)
    copy.wait()
    out_ref[...] = dot(hidden, down_ref[...]).astype(BF).reshape(out_ref.shape)


def staged(weight_delta, sketch_seed, up_weight, down_weight, norm_gain, state_pool, token_rows):
    learner = lax.axis_index(L)
    rows, cols = weight_delta.shape
    half = cols // 2
    width = 2 * rows
    count = state_pool.shape[0]
    out_rows = count // 16
    place = jnp.stack(
        [
            lax.axis_index("c"),
            lax.axis_index("zh"),
            lax.axis_index(Z),
            learner * cols,
            sketch_seed[0] * 7919,
            learner * out_rows,
        ]
    ).astype(jnp.int32)
    padded = half + RANK // 2
    part, kept, sent = call(
        range_kernel,
        ((16, rows // 16, RANK), (rows, padded), (rows, padded)),
        place,
        token_rows[:, 0, :],
        hbm=weight_delta,
        scratch=(pltpu.VMEM((rows, cols), F32),),
    )
    received = lax.ppermute(sent, "c", [(0, 1), (1, 0)])
    parts = swap(part, L)
    gain = norm_gain.astype(F32)[None]
    up_scratch = (pltpu.VMEM((width, cols), BF),)
    down_scratch = (pltpu.VMEM((half, 2 * width), BF),)
    gained, pool_up, squares = call(
        pool_kernel,
        ((count, width), (count, half), (2, count, RANK)),
        place, state_pool, gain,
        hbm=up_weight, scratch=up_scratch,
    )
    parts, received, gained, pool_up, squares, kept, place, gain, pool = lax.optimization_barrier(
        (parts, received, gained, pool_up, squares, kept, place, gain, state_pool)
    )
    spread, range_share = call(
        spread_kernel, ((32, rows // 16, RANK), (rows // 16, RANK)), place, parts
    )
    other_share = lax.ppermute(range_share, "zh", [(0, 1), (1, 0)])
    basis = swap(spread, CL)
    (pick,) = call(pick_kernel, ((2, 2 * count, count),), place, kept, received)
    (stacked,) = call(
        moved_kernel,
        ((16, count // 16, 2 * half + 2 * RANK),),
        place, basis, kept, received, gained, pool_up, squares,
    )
    (share,) = call(share_kernel, (stacked.shape,), place, swap(stacked, Z))
    gathered = swap(share, Z)
    step_part, coef, pool_pre = call(
        first_kernel,
        ((32, count // 16, width), (RANK, half), (count, half)),
        place, gathered,
        hbm=down_weight, scratch=down_scratch,
    )
    (spread,) = call(
        step_spread_kernel,
        ((*step_part.shape[:2], width + 2 * RANK),),
        place, swap(step_part, CL), other_share,
    )
    step = swap(spread, CL)
    stacked, own_second = call(
        second_kernel,
        ((8, count // 8, padded), (out_rows, 2 * width)),
        place, step, pool, gain, up_weight, basis, coef, pick,
    )
    (share,) = call(
        functools.partial(second_share_kernel, half), (stacked.shape,), place, swap(stacked, "zl")
    )
    (last,) = call(
        last_kernel,
        ((32, out_rows, 2 * width),),
        place, swap(share, "zl"), pool_pre, pick,
        hbm=down_weight, scratch=down_scratch,
    )
    last_share = jnp.sum(swap(last, CL).astype(F32), axis=0)
    return (own_second.astype(F32) + last_share).astype(BF)[None]


def solution(mesh):
    torus = Mesh(
        mesh.devices.reshape(4, 4, mesh.shape["rollout"], 2, 2), ("y", "x", "zl", "zh", "c")
    )
    return jax.shard_map(
        staged,
        mesh=torus,
        in_specs=(
            P(("zl", "zh", "c"), L),
            P(),
            P("zl", L),
            P(L, "zl"),
            P("zl"),
            P(None, "zl"),
            P(None, ("zh", "c"), None),
        ),
        out_specs=P(("zh", "c"), L, "zl"),
        check_vma=False,
    )
```

```python
import functools

import jax
import jax.numpy as jnp
from jax import lax
from jax.experimental import pallas as pl
from jax.experimental.pallas import tpu as pltpu
from jax.sharding import Mesh
from jax.sharding import PartitionSpec as P


D = 8192
RANK = 128
EPS = 1e-05
L = ("y", "x")
CL = ("c", "y", "x")
Z = ("zl", "zh")
BF = jnp.bfloat16
F32 = jnp.float32


def swap(x, axis):
    return lax.all_to_all(x, axis, split_axis=0, concat_axis=0, tiled=True)


def dot(a, b):
    return jnp.dot(a, b, preferred_element_type=F32)


def dot_t(a, b):
    return lax.dot_general(a, b, (((0,), (0,)), ((), ())), preferred_element_type=F32)


def hi_lo(x):
    hi = x.astype(BF).astype(F32)
    return hi, x - hi


def diagonal_offset(rows, first):
    row = first + lax.broadcasted_iota(jnp.int32, (rows, RANK), 0)
    col = lax.broadcasted_iota(jnp.int32, (rows, RANK), 1)
    return (col - row) & (RANK - 1)


def packed(gram, squares, offset):
    hi, lo = hi_lo(squares)
    rest = jnp.where(offset == RANK - 1, lo, jnp.where(offset == RANK - 2, hi, 0.0))
    return jnp.where(offset <= RANK // 2, gram, rest)


def unpacked_squares(gram, offset):
    return jnp.sum(jnp.where(offset >= RANK - 2, gram, 0.0), axis=1, keepdims=True)


def precise(a, b):
    return jnp.dot(a, b, precision=lax.Precision.HIGHEST, preferred_element_type=F32)


def silu(x):
    return x / (1.0 + jnp.exp(-x))


def total(ref):
    return jnp.sum(ref[...].astype(F32), axis=0)


HBM = pl.BlockSpec(memory_space=pltpu.HBM)
VMEM = pl.BlockSpec(memory_space=pltpu.VMEM)


def call(kernel, shapes, place, *arrays, hbm=None, scratch=(), limit=16):
    specs = [pl.BlockSpec(memory_space=pltpu.SMEM)]
    if hbm is not None:
        arrays = (hbm, *arrays)
        specs += [HBM]
        scratch = (*scratch, pltpu.SemaphoreType.DMA((2,)))
    specs += [VMEM] * (len(arrays) - (hbm is not None))
    return pl.pallas_call(
        kernel,
        out_shape=tuple(jax.ShapeDtypeStruct(shape, BF) for shape in shapes),
        in_specs=specs,
        out_specs=(VMEM,) * len(shapes),
        scratch_shapes=scratch,
        compiler_params=pltpu.CompilerParams(vmem_limit_bytes=int(limit * 1024 * 1024)),
    )(place, *arrays)


def column(row):
    return jnp.broadcast_to(row, (RANK, RANK)).T


def chosen(tokens, step):
    count = tokens.shape[0] // 2
    rows = tokens[step * count : (step + 1) * count].astype(F32)
    lane = lax.broadcasted_iota(jnp.int32, (count, RANK), 1).astype(F32)
    return jnp.where(rows == lane, 1.0, 0.0).astype(BF)


def picks(place, kept_ref, got_ref, step):
    half = kept_ref.shape[1] - RANK // 2
    mine = chosen(kept_ref[:, half : half + 1], step)
    theirs = chosen(got_ref[:, half : half + 1], step)
    first = place[0] == 0
    return jnp.concatenate(
        [jnp.where(first, mine, theirs), jnp.where(first, theirs, mine)], axis=0
    )


def own_half(place, x):
    half = x.shape[1] // 2
    return jnp.where(place[0] == 0, x[:, :half], x[:, half:])


def range_kernel(place, delta_hbm, part_ref, delta_ref, sem):
    rows, cols = delta_ref.shape
    split = rows // 2
    copies = [
        pltpu.make_async_copy(
            delta_hbm.at[pl.ds(i * split, split)], delta_ref.at[pl.ds(i * split, split)], sem.at[i]
        )
        for i in range(2)
    ]
    for copy in copies:
        copy.start()
    row_index = place[3] + lax.broadcasted_iota(jnp.int32, (cols, RANK), 0)
    col_index = lax.broadcasted_iota(jnp.int32, (cols, RANK), 1)
    hashed = row_index * RANK + col_index + place[4]
    hashed = hashed * 1103515245 + 12345
    hashed = hashed ^ lax.shift_right_logical(hashed, jnp.int32(16))
    hashed = hashed * 73244475
    hashed = hashed ^ lax.shift_right_logical(hashed, jnp.int32(15))
    parity = lax.shift_right_logical(hashed, jnp.int32(11)) & 1
    signs = (2 * parity - 1).astype(F32).astype(BF)
    for i, copy in enumerate(copies):
        copy.wait()
        span = slice(i * split, (i + 1) * split)
        delta = delta_ref[span].astype(BF)
        parts = part_ref.shape[0] // 2
        part_ref[i * parts : (i + 1) * parts] = (
            dot(delta, signs).astype(BF).reshape(parts, *part_ref.shape[1:])
        )


def halves_kernel(place, delta_ref, tokens_ref, kept_ref, sent_ref):
    core = place[0]
    half = delta_ref.shape[1] // 2
    delta = delta_ref[...].astype(BF)
    left, right = delta[:, :half], delta[:, half:]
    tokens = jnp.concatenate([column(tokens_ref[i : i + 1].astype(F32)) for i in range(2)], axis=0)
    tokens = tokens[:, : RANK // 2].astype(BF)
    kept_ref[...] = jnp.concatenate([jnp.where(core == 0, left, right), tokens], axis=1)
    sent_ref[...] = jnp.concatenate([jnp.where(core == 0, right, left), tokens], axis=1)


def pick_kernel(place, kept_ref, got_ref, pick_ref):
    for step in range(2):
        pick_ref[step] = picks(place, kept_ref, got_ref, step)


def pool_kernel(place, up_hbm, pool_ref, gain_ref, gained_ref, up_out_ref, squares_ref, up_ref, sem):
    z_half = place[1]
    width = up_ref.shape[0]
    first = pl.multiple_of(z_half * width, width)
    copy = pltpu.make_async_copy(up_hbm.at[pl.ds(first, width)], up_ref, sem.at[0])
    copy.start()
    pool = jnp.where(z_half == 0, pool_ref[:, :width], pool_ref[:, width:]).astype(F32)
    gain = jnp.where(z_half == 0, gain_ref[:, :width], gain_ref[:, width:])
    gained = (pool * gain).astype(BF)
    gained_ref[...] = gained
    squares = jnp.broadcast_to(jnp.sum(pool * pool, axis=1, keepdims=True), (pool.shape[0], RANK))
    hi, lo = hi_lo(squares)
    squares_ref[0] = hi.astype(BF)
    squares_ref[1] = lo.astype(BF)
    copy.wait()
    up_out_ref[...] = own_half(place, dot(gained, up_ref[...])).astype(BF)


def spread_kernel(place, parts_ref, out_ref):
    out_ref[...] = jnp.broadcast_to(total(parts_ref).astype(BF), out_ref.shape)


def moved_kernel(place, basis_ref, kept_ref, got_ref, pool_ref, up_ref, squares_ref, out_ref):
    core = place[0]
    rows, wide = kept_ref.shape
    half = wide - RANK // 2
    count = basis_ref.shape[0] // 2
    own = basis_ref[pl.ds(core * count, count)].reshape(rows, RANK)
    other = basis_ref[pl.ds((1 - core) * count, count)].reshape(rows, RANK)
    basis = basis_ref[...].reshape(2 * rows, RANK)

    def put(first, values):
        values = values.astype(BF)
        out_ref[:, :, first : first + values.shape[1]] = values.reshape(
            *out_ref.shape[:2], values.shape[1]
        )

    moved = dot_t(own, kept_ref[...]) + dot_t(other, got_ref[...])
    put(0, jnp.concatenate([moved[:, :half].astype(BF), up_ref[...]], axis=1))
    squares = squares_ref[0].astype(F32) + squares_ref[1].astype(F32)
    put(2 * half, packed(dot_t(basis, basis), squares, diagonal_offset(RANK, 0)))
    put(2 * half + RANK, dot(pool_ref[...], basis))


def share_kernel(place, parts_ref, out_ref):
    share = total(parts_ref)
    rows, width = share.shape
    first = width - 2 * RANK
    offset = diagonal_offset(rows, place[2] * rows)
    gram = share[:, first : first + RANK]
    gram = packed(gram, unpacked_squares(gram, offset), offset)
    share = jnp.concatenate([share[:, :first], gram, share[:, first + RANK :]], axis=1)
    out_ref[...] = jnp.broadcast_to(share.astype(BF), out_ref.shape)


def down_copy(place, down_hbm, down_ref, sem):
    half = down_ref.shape[0]
    first = pl.multiple_of(place[0] * half, RANK // 2)
    return pltpu.make_async_copy(down_hbm.at[pl.ds(first, half)], down_ref, sem.at[0])


def first_kernel(place, down_hbm, z_ref, step_ref, coef_ref, pre_ref, down_ref, sem):
    copy = down_copy(place, down_hbm, down_ref, sem)
    copy.start()
    half = coef_ref.shape[1]
    gathered = z_ref[...].reshape(RANK, z_ref.shape[2])
    gram = gathered[:, 2 * half : 2 * half + RANK].astype(F32)
    row = lax.broadcasted_iota(jnp.int32, (RANK, RANK), 0)
    col = lax.broadcasted_iota(jnp.int32, (RANK, RANK), 1)
    offset = (col - row) & (RANK - 1)
    squares = unpacked_squares(gram, offset)
    gram = jnp.where(offset <= RANK // 2, gram, gram.T)
    eye = jnp.where(row == col, 1.0, 0.0)
    on_diag = gram * eye
    scale_col = lax.rsqrt(jnp.sum(on_diag, axis=1, keepdims=True))
    scale_row = lax.rsqrt(jnp.sum(on_diag, axis=0, keepdims=True))
    unit = gram * scale_col * scale_row
    bound = jnp.max(jnp.sum(jnp.abs(unit), axis=1, keepdims=True), axis=0, keepdims=True)
    step = 2.0 / (1.0 + bound)
    start = step * (2.0 * eye - step * unit)

    def going(state):
        count, error, _ = state
        return jnp.logical_and(count < 40, error > 2e-4)

    def refine(state):
        count, _, inverse = state
        left = eye - precise(unit, inverse)
        moved = dot(inverse.astype(BF), left.astype(BF))
        return count + 1, jnp.sum(left * left), inverse + moved

    _, _, inverse = lax.while_loop(going, refine, (0, jnp.float32(1.0), start))
    hi, lo = hi_lo(inverse * scale_col * scale_row)
    moved = gathered[:, :half]
    coef = (dot(hi.astype(BF), moved) + dot(lo.astype(BF), moved)).astype(BF)
    coef_ref[...] = coef
    pre = gathered[:, half : 2 * half].astype(F32) + dot(gathered[:, 2 * half + RANK :], coef)
    pre_ref[...] = pre.astype(BF)
    hidden = silu(pre * lax.rsqrt(squares / D + EPS)).astype(BF)
    copy.wait()
    result = dot(hidden, down_ref[...]).astype(BF)
    count, rows, width = step_ref.shape
    step_ref[: count // 2] = result[:, :width].reshape(count // 2, rows, width)
    step_ref[count // 2 :] = result[:, width:].reshape(count // 2, rows, width)


def second_kernel(
    place, up_hbm, step_ref, pool_ref, gain_ref, basis_ref, coef_ref, pick_ref, out_ref, rows_ref, up_ref, sem
):
    z_half = place[1]
    _, _, width = step_ref.shape
    pool_rows = pool_ref.shape[0]
    start = pl.multiple_of(z_half * width, width)
    copy = pltpu.make_async_copy(up_hbm.at[pl.ds(start, width)], up_ref, sem.at[0])
    copy.start()
    half = coef_ref.shape[1]
    basis = basis_ref[...].reshape(width, RANK)
    step = step_ref[...].astype(F32).reshape(2, pool_rows, width)
    pool = pool_ref[...]
    left = (pool[:, :width].astype(F32) + step[0]).astype(BF)
    right = (pool[:, width:].astype(F32) + step[1]).astype(BF)
    carried = jnp.concatenate([left, right], axis=1)
    gain = jnp.where(z_half == 0, gain_ref[:, :width], gain_ref[:, width:])
    gained = (jnp.where(z_half == 0, left, right).astype(F32) * gain).astype(BF)

    def second(one, two):
        return (dot(one, carried) + dot(two, pool)).astype(BF)

    wide = second(pick_ref[0], pick_ref[1]).astype(F32)
    squares = jnp.sum(wide * wide, axis=1, keepdims=True)
    row = lax.broadcasted_iota(jnp.int32, (rows_ref.shape[0], pool_rows), 0)
    lane = lax.broadcasted_iota(jnp.int32, (rows_ref.shape[0], pool_rows), 1)
    here = jnp.where(lane == row + place[5], 1.0, 0.0).astype(BF)
    own = [
        dot(here, jnp.where(place[0] == 0, pick_ref[i, :pool_rows], pick_ref[i, pool_rows:]))
        for i in range(2)
    ]
    rows_ref[...] = second(own[0].astype(BF), own[1].astype(BF))
    lane = lax.broadcasted_iota(jnp.int32, (pool_rows, out_ref.shape[2] - half), 1)
    first = 4 * z_half
    tail = jnp.zeros(lane.shape, F32)
    for place_in, value in enumerate((*hi_lo(squares[:pool_rows]), *hi_lo(squares[pool_rows:]))):
        tail = jnp.where(lane == first + place_in, value, tail)
    low = dot(dot(gained, basis).astype(BF), coef_ref[...])
    copy.wait()
    up = own_half(place, dot(gained, up_ref[...])) + low
    both = jnp.concatenate([up.astype(BF), tail.astype(BF)], axis=1)
    out_ref[...] = both.reshape(out_ref.shape)


def second_share_kernel(half, place, parts_ref, out_ref):
    share = total(parts_ref)
    lane = lax.broadcasted_iota(jnp.int32, share.shape, 1)
    out = share
    for first in range(half, half + 8, 2):
        whole = jnp.where(jnp.logical_or(lane == first, lane == first + 1), share, 0.0)
        hi, lo = hi_lo(jnp.sum(whole, axis=1, keepdims=True))
        out = jnp.where(lane == first, hi, jnp.where(lane == first + 1, lo, out))
    out_ref[...] = jnp.broadcast_to(out.astype(BF), out_ref.shape)


def last_kernel(place, down_hbm, z_ref, pre_ref, pick_ref, out_ref, down_ref, sem):
    copy = down_copy(place, down_hbm, down_ref, sem)
    copy.start()
    z_half = place[1]
    half = pre_ref.shape[1]
    pool_rows = pre_ref.shape[0]
    gathered = z_ref[...].reshape(pool_rows, z_ref.shape[2])
    lane = lax.broadcasted_iota(jnp.int32, gathered.shape, 1)

    def squares(first):
        first = half + 4 * z_half + first
        chosen = jnp.logical_or(lane == first, lane == first + 1)
        return jnp.sum(jnp.where(chosen, gathered.astype(F32), 0.0), axis=1, keepdims=True)

    scale = lax.rsqrt(jnp.concatenate([squares(0), squares(2)], axis=0) / D + EPS)
    pre = dot(pick_ref[0], gathered[:, :half]) + dot(pick_ref[1], pre_ref[...])
    hidden = silu(pre * scale).astype(BF)
    copy.wait()
    out_ref[...] = dot(hidden, down_ref[...]).astype(BF).reshape(out_ref.shape)


def staged(weight_delta, sketch_seed, up_weight, down_weight, norm_gain, state_pool, token_rows):
    learner = lax.axis_index(L)
    rows, cols = weight_delta.shape
    half = cols // 2
    width = 2 * rows
    count = state_pool.shape[0]
    out_rows = count // 16
    place = jnp.stack(
        [
            lax.axis_index("c"),
            lax.axis_index("zh"),
            lax.axis_index(Z),
            learner * cols,
            sketch_seed[0] * 7919,
            learner * out_rows,
        ]
    ).astype(jnp.int32)
    padded = half + RANK // 2
    (part,) = call(
        range_kernel,
        ((16, rows // 16, RANK),),
        place,
        hbm=weight_delta,
        scratch=(pltpu.VMEM((rows, cols), F32),),
        limit=63.5,
    )
    kept, sent = call(
        halves_kernel, ((rows, padded), (rows, padded)), place, weight_delta, token_rows[:, 0, :]
    )
    received = lax.ppermute(sent, "c", [(0, 1), (1, 0)])
    parts = swap(part, L)
    gain = norm_gain.astype(F32)[None]
    up_scratch = (pltpu.VMEM((width, cols), BF),)
    down_scratch = (pltpu.VMEM((half, 2 * width), BF),)
    parts, place, gain, pool = lax.optimization_barrier((parts, place, gain, state_pool))
    (spread,) = call(spread_kernel, ((32, rows // 16, RANK),), place, parts)
    basis = swap(spread, CL)
    (pick,) = call(pick_kernel, ((2, 2 * count, count),), place, kept, received)
    gained, pool_up, squares = call(
        pool_kernel,
        ((count, width), (count, half), (2, count, RANK)),
        place, pool, gain,
        hbm=up_weight, scratch=up_scratch,
    )
    (stacked,) = call(
        moved_kernel,
        ((16, count // 16, 2 * half + 2 * RANK),),
        place, basis, kept, received, gained, pool_up, squares,
    )
    (share,) = call(share_kernel, (stacked.shape,), place, swap(stacked, Z))
    step_part, coef, pool_pre = call(
        first_kernel,
        ((32, count // 16, width), (RANK, half), (count, half)),
        place, swap(share, Z),
        hbm=down_weight, scratch=down_scratch,
    )
    (spread,) = call(spread_kernel, (step_part.shape,), place, swap(step_part, CL))
    step = swap(spread, CL)
    stacked, own_second = call(
        second_kernel,
        ((16, count // 16, padded), (out_rows, 2 * width)),
        place, step, pool, gain, basis, coef, pick,
        hbm=up_weight, scratch=up_scratch,
    )
    (share,) = call(
        functools.partial(second_share_kernel, half), (stacked.shape,), place, swap(stacked, Z)
    )
    (last,) = call(
        last_kernel,
        ((32, out_rows, 2 * width),),
        place, swap(share, Z), pool_pre, pick,
        hbm=down_weight, scratch=down_scratch,
    )
    last_share = jnp.sum(swap(last, CL).astype(F32), axis=0)
    return (own_second.astype(F32) + last_share).astype(BF)[None]


def solution(mesh):
    torus = Mesh(
        mesh.devices.reshape(4, 4, mesh.shape["rollout"], 2, 2), ("y", "x", "zl", "zh", "c")
    )
    return jax.shard_map(
        staged,
        mesh=torus,
        in_specs=(
            P(("zl", "zh", "c"), L),
            P(),
            P("zl", L),
            P(L, "zl"),
            P("zl"),
            P(None, "zl"),
            P(None, ("zh", "c"), None),
        ),
        out_specs=P(("zh", "c"), L, "zl"),
        check_vma=False,
    )
```

```python
import functools

import jax
import jax.numpy as jnp
from jax import lax
from jax.experimental import pallas as pl
from jax.experimental.pallas import tpu as pltpu
from jax.sharding import Mesh
from jax.sharding import PartitionSpec as P


D = 8192
RANK = 128
EPS = 1e-05
L = ("y", "x")
CL = ("c", "y", "x")
Z = ("zl", "zh")
BF = jnp.bfloat16
F32 = jnp.float32


def swap(x, axis):
    return lax.all_to_all(x, axis, split_axis=0, concat_axis=0, tiled=True)


def dot(a, b):
    return jnp.dot(a, b, preferred_element_type=F32)


def dot_t(a, b):
    return lax.dot_general(a, b, (((0,), (0,)), ((), ())), preferred_element_type=F32)


def hi_lo(x):
    hi = x.astype(BF).astype(F32)
    return hi, x - hi


def diagonal_offset(rows, first):
    row = first + lax.broadcasted_iota(jnp.int32, (rows, RANK), 0)
    col = lax.broadcasted_iota(jnp.int32, (rows, RANK), 1)
    return (col - row) & (RANK - 1)


def packed(gram, squares, offset):
    hi, lo = hi_lo(squares)
    rest = jnp.where(offset == RANK - 1, lo, jnp.where(offset == RANK - 2, hi, 0.0))
    return jnp.where(offset <= RANK // 2, gram, rest)


def unpacked_squares(gram, offset):
    return jnp.sum(jnp.where(offset >= RANK - 2, gram, 0.0), axis=1, keepdims=True)


def precise(a, b):
    return jnp.dot(a, b, precision=lax.Precision.HIGHEST, preferred_element_type=F32)


def silu(x):
    return x / (1.0 + jnp.exp(-x))


def total(ref):
    return jnp.sum(ref[...].astype(F32), axis=0)


HBM = pl.BlockSpec(memory_space=pltpu.HBM)
VMEM = pl.BlockSpec(memory_space=pltpu.VMEM)


def call(kernel, shapes, place, *arrays, hbm=None, scratch=()):
    specs = [pl.BlockSpec(memory_space=pltpu.SMEM)]
    if hbm is not None:
        arrays = (hbm, *arrays)
        specs += [HBM]
        scratch = (*scratch, pltpu.SemaphoreType.DMA((2,)))
    specs += [VMEM] * (len(arrays) - (hbm is not None))
    return pl.pallas_call(
        kernel,
        out_shape=tuple(jax.ShapeDtypeStruct(shape, BF) for shape in shapes),
        in_specs=specs,
        out_specs=(VMEM,) * len(shapes),
        scratch_shapes=scratch,
        compiler_params=pltpu.CompilerParams(vmem_limit_bytes=16 * 1024 * 1024),
    )(place, *arrays)


def column(row):
    return jnp.broadcast_to(row, (RANK, RANK)).T


def chosen(tokens, step):
    count = tokens.shape[0] // 2
    rows = tokens[step * count : (step + 1) * count].astype(F32)
    lane = lax.broadcasted_iota(jnp.int32, (count, RANK), 1).astype(F32)
    return jnp.where(rows == lane, 1.0, 0.0).astype(BF)


def picks(place, kept_ref, got_ref, step):
    half = kept_ref.shape[1] - RANK // 2
    mine = chosen(kept_ref[:, half : half + 1], step)
    theirs = chosen(got_ref[:, half : half + 1], step)
    first = place[0] == 0
    return jnp.concatenate(
        [jnp.where(first, mine, theirs), jnp.where(first, theirs, mine)], axis=0
    )


def own_half(place, x):
    half = x.shape[1] // 2
    return jnp.where(place[0] == 0, x[:, :half], x[:, half:])


def range_kernel(place, delta_hbm, tokens_ref, part_ref, kept_ref, sent_ref, delta_ref, sem):
    core = place[0]
    rows, cols = delta_ref.shape
    half = cols // 2
    split = rows // 2
    copies = [
        pltpu.make_async_copy(
            delta_hbm.at[pl.ds(i * split, split)], delta_ref.at[pl.ds(i * split, split)], sem.at[i]
        )
        for i in range(2)
    ]
    for copy in copies:
        copy.start()
    row_index = place[3] + lax.broadcasted_iota(jnp.int32, (cols, RANK), 0)
    col_index = lax.broadcasted_iota(jnp.int32, (cols, RANK), 1)
    hashed = row_index * RANK + col_index + place[4]
    hashed = hashed * 1103515245 + 12345
    hashed = hashed ^ lax.shift_right_logical(hashed, jnp.int32(16))
    hashed = hashed * 73244475
    hashed = hashed ^ lax.shift_right_logical(hashed, jnp.int32(15))
    parity = lax.shift_right_logical(hashed, jnp.int32(11)) & 1
    signs = (2 * parity - 1).astype(F32).astype(BF)
    for i, copy in enumerate(copies):
        copy.wait()
        span = slice(i * split, (i + 1) * split)
        delta = delta_ref[span].astype(BF)
        parts = part_ref.shape[0] // 2
        part_ref[i * parts : (i + 1) * parts] = (
            dot(delta, signs).astype(BF).reshape(parts, *part_ref.shape[1:])
        )
        left, right = delta[:, :half], delta[:, half:]
        tokens = column(tokens_ref[i : i + 1].astype(F32))[:, : RANK // 2].astype(BF)
        kept_ref[span] = jnp.concatenate([jnp.where(core == 0, left, right), tokens], axis=1)
        sent_ref[span] = jnp.concatenate([jnp.where(core == 0, right, left), tokens], axis=1)


def pick_kernel(place, kept_ref, got_ref, pick_ref):
    for step in range(2):
        pick_ref[step] = picks(place, kept_ref, got_ref, step)


def pool_kernel(place, up_hbm, pool_ref, gain_ref, gained_ref, up_out_ref, squares_ref, up_ref, sem):
    z_half = place[1]
    width = up_ref.shape[0]
    first = pl.multiple_of(z_half * width, width)
    copy = pltpu.make_async_copy(up_hbm.at[pl.ds(first, width)], up_ref, sem.at[0])
    copy.start()
    pool = jnp.where(z_half == 0, pool_ref[:, :width], pool_ref[:, width:]).astype(F32)
    gain = jnp.where(z_half == 0, gain_ref[:, :width], gain_ref[:, width:])
    gained = (pool * gain).astype(BF)
    gained_ref[...] = gained
    squares = jnp.broadcast_to(jnp.sum(pool * pool, axis=1, keepdims=True), (pool.shape[0], RANK))
    hi, lo = hi_lo(squares)
    squares_ref[0] = hi.astype(BF)
    squares_ref[1] = lo.astype(BF)
    copy.wait()
    up_out_ref[...] = own_half(place, dot(gained, up_ref[...])).astype(BF)


def spread_kernel(place, parts_ref, out_ref):
    out_ref[...] = jnp.broadcast_to(total(parts_ref).astype(BF), out_ref.shape)


def moved_kernel(place, basis_ref, kept_ref, got_ref, pool_ref, up_ref, squares_ref, out_ref):
    core = place[0]
    rows, wide = kept_ref.shape
    half = wide - RANK // 2
    count = basis_ref.shape[0] // 2
    own = basis_ref[pl.ds(core * count, count)].reshape(rows, RANK)
    other = basis_ref[pl.ds((1 - core) * count, count)].reshape(rows, RANK)
    basis = basis_ref[...].reshape(2 * rows, RANK)

    def put(first, values):
        values = values.astype(BF)
        out_ref[:, :, first : first + values.shape[1]] = values.reshape(
            *out_ref.shape[:2], values.shape[1]
        )

    moved = dot_t(own, kept_ref[...]) + dot_t(other, got_ref[...])
    put(0, jnp.concatenate([moved[:, :half].astype(BF), up_ref[...]], axis=1))
    squares = squares_ref[0].astype(F32) + squares_ref[1].astype(F32)
    put(2 * half, packed(dot_t(basis, basis), squares, diagonal_offset(RANK, 0)))
    put(2 * half + RANK, dot(pool_ref[...], basis))


def share_kernel(place, parts_ref, out_ref):
    share = total(parts_ref)
    rows, width = share.shape
    first = width - 2 * RANK
    offset = diagonal_offset(rows, place[2] * rows)
    gram = share[:, first : first + RANK]
    gram = packed(gram, unpacked_squares(gram, offset), offset)
    share = jnp.concatenate([share[:, :first], gram, share[:, first + RANK :]], axis=1)
    out_ref[...] = jnp.broadcast_to(share.astype(BF), out_ref.shape)


def down_copy(place, down_hbm, down_ref, sem):
    half = down_ref.shape[0]
    first = pl.multiple_of(place[0] * half, RANK // 2)
    return pltpu.make_async_copy(down_hbm.at[pl.ds(first, half)], down_ref, sem.at[0])


def first_kernel(place, down_hbm, z_ref, step_ref, coef_ref, pre_ref, down_ref, sem):
    copy = down_copy(place, down_hbm, down_ref, sem)
    copy.start()
    half = coef_ref.shape[1]
    gathered = z_ref[...].reshape(RANK, z_ref.shape[2])
    gram = gathered[:, 2 * half : 2 * half + RANK].astype(F32)
    row = lax.broadcasted_iota(jnp.int32, (RANK, RANK), 0)
    col = lax.broadcasted_iota(jnp.int32, (RANK, RANK), 1)
    offset = (col - row) & (RANK - 1)
    squares = unpacked_squares(gram, offset)
    gram = jnp.where(offset <= RANK // 2, gram, gram.T)
    eye = jnp.where(row == col, 1.0, 0.0)
    on_diag = gram * eye
    scale_col = lax.rsqrt(jnp.sum(on_diag, axis=1, keepdims=True))
    scale_row = lax.rsqrt(jnp.sum(on_diag, axis=0, keepdims=True))
    unit = gram * scale_col * scale_row
    bound = jnp.max(jnp.sum(jnp.abs(unit), axis=1, keepdims=True), axis=0, keepdims=True)
    step = 2.0 / (1.0 + bound)
    start = step * (2.0 * eye - step * unit)

    def going(state):
        count, error, _ = state
        return jnp.logical_and(count < 40, error > 2e-4)

    def refine(state):
        count, _, inverse = state
        left = eye - precise(unit, inverse)
        moved = dot(inverse.astype(BF), left.astype(BF))
        return count + 1, jnp.sum(left * left), inverse + moved

    _, _, inverse = lax.while_loop(going, refine, (0, jnp.float32(1.0), start))
    hi, lo = hi_lo(inverse * scale_col * scale_row)
    moved = gathered[:, :half]
    coef = (dot(hi.astype(BF), moved) + dot(lo.astype(BF), moved)).astype(BF)
    coef_ref[...] = coef
    pre = gathered[:, half : 2 * half].astype(F32) + dot(gathered[:, 2 * half + RANK :], coef)
    pre_ref[...] = pre.astype(BF)
    hidden = silu(pre * lax.rsqrt(squares / D + EPS)).astype(BF)
    copy.wait()
    result = dot(hidden, down_ref[...]).astype(BF)
    count, rows, width = step_ref.shape
    step_ref[: count // 2] = result[:, :width].reshape(count // 2, rows, width)
    step_ref[count // 2 :] = result[:, width:].reshape(count // 2, rows, width)


def second_kernel(
    place, up_hbm, step_ref, pool_ref, gain_ref, basis_ref, coef_ref, pick_ref, out_ref, rows_ref, up_ref, sem
):
    z_half = place[1]
    _, _, width = step_ref.shape
    pool_rows = pool_ref.shape[0]
    start = pl.multiple_of(z_half * width, width)
    copy = pltpu.make_async_copy(up_hbm.at[pl.ds(start, width)], up_ref, sem.at[0])
    copy.start()
    half = coef_ref.shape[1]
    basis = basis_ref[...].reshape(width, RANK)
    step = step_ref[...].astype(F32).reshape(2, pool_rows, width)
    pool = pool_ref[...]
    left = (pool[:, :width].astype(F32) + step[0]).astype(BF)
    right = (pool[:, width:].astype(F32) + step[1]).astype(BF)
    carried = jnp.concatenate([left, right], axis=1)
    gain = jnp.where(z_half == 0, gain_ref[:, :width], gain_ref[:, width:])
    gained = (jnp.where(z_half == 0, left, right).astype(F32) * gain).astype(BF)

    def second(one, two):
        return (dot(one, carried) + dot(two, pool)).astype(BF)

    wide = second(pick_ref[0], pick_ref[1]).astype(F32)
    squares = jnp.sum(wide * wide, axis=1, keepdims=True)
    row = lax.broadcasted_iota(jnp.int32, (rows_ref.shape[0], pool_rows), 0)
    lane = lax.broadcasted_iota(jnp.int32, (rows_ref.shape[0], pool_rows), 1)
    here = jnp.where(lane == row + place[5], 1.0, 0.0).astype(BF)
    own = [
        dot(here, jnp.where(place[0] == 0, pick_ref[i, :pool_rows], pick_ref[i, pool_rows:]))
        for i in range(2)
    ]
    rows_ref[...] = second(own[0].astype(BF), own[1].astype(BF))
    lane = lax.broadcasted_iota(jnp.int32, (pool_rows, out_ref.shape[2] - half), 1)
    first = 4 * z_half
    tail = jnp.zeros(lane.shape, F32)
    for place_in, value in enumerate((*hi_lo(squares[:pool_rows]), *hi_lo(squares[pool_rows:]))):
        tail = jnp.where(lane == first + place_in, value, tail)
    low = dot(dot(gained, basis).astype(BF), coef_ref[...])
    copy.wait()
    up = own_half(place, dot(gained, up_ref[...])) + low
    both = jnp.concatenate([up.astype(BF), tail.astype(BF)], axis=1)
    out_ref[...] = both.reshape(out_ref.shape)


def second_share_kernel(half, place, parts_ref, out_ref):
    share = total(parts_ref)
    lane = lax.broadcasted_iota(jnp.int32, share.shape, 1)
    out = share
    for first in range(half, half + 8, 2):
        whole = jnp.where(jnp.logical_or(lane == first, lane == first + 1), share, 0.0)
        hi, lo = hi_lo(jnp.sum(whole, axis=1, keepdims=True))
        out = jnp.where(lane == first, hi, jnp.where(lane == first + 1, lo, out))
    out_ref[...] = jnp.broadcast_to(out.astype(BF), out_ref.shape)


def last_kernel(place, down_hbm, z_ref, pre_ref, pick_ref, out_ref, down_ref, sem):
    copy = down_copy(place, down_hbm, down_ref, sem)
    copy.start()
    z_half = place[1]
    half = pre_ref.shape[1]
    pool_rows = pre_ref.shape[0]
    gathered = z_ref[...].reshape(pool_rows, z_ref.shape[2])
    lane = lax.broadcasted_iota(jnp.int32, gathered.shape, 1)

    def squares(first):
        first = half + 4 * z_half + first
        chosen = jnp.logical_or(lane == first, lane == first + 1)
        return jnp.sum(jnp.where(chosen, gathered.astype(F32), 0.0), axis=1, keepdims=True)

    scale = lax.rsqrt(jnp.concatenate([squares(0), squares(2)], axis=0) / D + EPS)
    pre = dot(pick_ref[0], gathered[:, :half]) + dot(pick_ref[1], pre_ref[...])
    hidden = silu(pre * scale).astype(BF)
    copy.wait()
    out_ref[...] = dot(hidden, down_ref[...]).astype(BF).reshape(out_ref.shape)


def staged(weight_delta, sketch_seed, up_weight, down_weight, norm_gain, state_pool, token_rows):
    learner = lax.axis_index(L)
    rows, cols = weight_delta.shape
    half = cols // 2
    width = 2 * rows
    count = state_pool.shape[0]
    out_rows = count // 16
    place = jnp.stack(
        [
            lax.axis_index("c"),
            lax.axis_index("zh"),
            lax.axis_index(Z),
            learner * cols,
            sketch_seed[0] * 7919,
            learner * out_rows,
        ]
    ).astype(jnp.int32)
    padded = half + RANK // 2
    part, kept, sent = call(
        range_kernel,
        ((16, rows // 16, RANK), (rows, padded), (rows, padded)),
        place,
        token_rows[:, 0, :],
        hbm=weight_delta,
        scratch=(pltpu.VMEM((rows, cols), F32),),
    )
    received = lax.ppermute(sent, "c", [(0, 1), (1, 0)])
    parts = swap(part, L)
    gain = norm_gain.astype(F32)[None]
    up_scratch = (pltpu.VMEM((width, cols), BF),)
    down_scratch = (pltpu.VMEM((half, 2 * width), BF),)
    parts, place, gain, pool = lax.optimization_barrier((parts, place, gain, state_pool))
    (spread,) = call(spread_kernel, ((32, rows // 16, RANK),), place, parts)
    basis = swap(spread, CL)
    (pick,) = call(pick_kernel, ((2, 2 * count, count),), place, kept, received)
    gained, pool_up, squares = call(
        pool_kernel,
        ((count, width), (count, half), (2, count, RANK)),
        place, pool, gain,
        hbm=up_weight, scratch=up_scratch,
    )
    (stacked,) = call(
        moved_kernel,
        ((16, count // 16, 2 * half + 2 * RANK),),
        place, basis, kept, received, gained, pool_up, squares,
    )
    (share,) = call(share_kernel, (stacked.shape,), place, swap(stacked, Z))
    step_part, coef, pool_pre = call(
        first_kernel,
        ((32, count // 16, width), (RANK, half), (count, half)),
        place, swap(share, Z),
        hbm=down_weight, scratch=down_scratch,
    )
    (spread,) = call(spread_kernel, (step_part.shape,), place, swap(step_part, CL))
    step = swap(spread, CL)
    stacked, own_second = call(
        second_kernel,
        ((16, count // 16, padded), (out_rows, 2 * width)),
        place, step, pool, gain, basis, coef, pick,
        hbm=up_weight, scratch=up_scratch,
    )
    (share,) = call(
        functools.partial(second_share_kernel, half), (stacked.shape,), place, swap(stacked, Z)
    )
    (last,) = call(
        last_kernel,
        ((32, out_rows, 2 * width),),
        place, swap(share, Z), pool_pre, pick,
        hbm=down_weight, scratch=down_scratch,
    )
    last_share = jnp.sum(swap(last, CL).astype(F32), axis=0)
    return (own_second.astype(F32) + last_share).astype(BF)[None]


def solution(mesh):
    torus = Mesh(
        mesh.devices.reshape(4, 4, mesh.shape["rollout"], 2, 2), ("y", "x", "zl", "zh", "c")
    )
    return jax.shard_map(
        staged,
        mesh=torus,
        in_specs=(
            P(("zl", "zh", "c"), L),
            P(),
            P("zl", L),
            P(L, "zl"),
            P("zl"),
            P(None, "zl"),
            P(None, ("zh", "c"), None),
        ),
        out_specs=P(("zh", "c"), L, "zl"),
        check_vma=False,
    )
```
